32 devices in a mesh: pairs: 2 (over x), ctx: 16 (over z, y, core).
Axes of the slice: x: 2, y: 2, z: 4, core: 2. Of those that a mesh axis runs over, the one named last changes fastest.
Arguments:
- prompt_keys: bfloat16 [1024, 512], P(('pairs', 'ctx')), parts along dimension 0, may hold values from -4 to 4
- prompt_values: bfloat16 [1024, 512], P(('pairs', 'ctx')), parts along dimension 0, may hold values from -6 to 6
- queries: bfloat16 [4, 768, 4096], P('pairs', 'ctx'), parts along dimension 0, may hold values from -100 to 100
- resp_keys: bfloat16 [4, 768, 512], P('pairs', 'ctx'), parts along dimension 0, may hold values from -6 to 6
- resp_values: bfloat16 [4, 768, 512], P('pairs', 'ctx'), parts along dimension 0, may hold values from -6 to 6
- cotangent: bfloat16 [4, 768, 4096], P('pairs', 'ctx'), parts along dimension 0, may hold values from -48 to 48
- lengths: int32 [4], P('pairs'), parts along dimension 0, may hold values from 192 to 768, as said below
Outputs:
- grad_queries: float32 [4, 768, 4096], P('pairs', 'ctx'), parts along dimension 0
- grad_resp_keys: float32 [4, 768, 512], P('pairs', 'ctx'), parts along dimension 0
- grad_resp_values: float32 [4, 768, 512], P('pairs', 'ctx'), parts along dimension 0
- grad_prompt_keys: float32 [1024, 512], P(('pairs', 'ctx')), parts along dimension 0
- grad_prompt_values: float32 [1024, 512], P(('pairs', 'ctx')), parts along dimension 0
The draws below stay inside these ranges and needn't reach their ends.
There are 2 independent parts, one for each index of `pairs`. The reference program is written for one: setup_inputs(seed, part) draws one part's arguments, and reference() takes and returns one part's arrays. A program takes and returns all parts, laid end to end along the dimension named above; each array names one. Nothing has to cross between parts.
Inputs may be any that keep to these rules, and one draw needn't show every extreme that they name: `lengths`: in every pair one of the two responses has all 768 rows live.
All inputs are finite; a program needn't handle non-finite values.
Results may differ from the reference program's by a relative error of at most 0.005.
Values may be sent and summed in bfloat16 or wider, within the bound.
A program may use at most 128 MiB of HBM per device.

```python
import math
import jax
import jax.numpy as jnp
from jax import lax

HEADS = 32
KV_HEADS = 4
HEAD_DIM = 128
RESP = 768
PROMPT = 512


def prompt_draw(key):
    return jax.random.truncated_normal(jax.random.fold_in(key, 11), -4.0, 4.0, (PROMPT, KV_HEADS * HEAD_DIM), jnp.float32)


def draw_prompt_keys(key, part):
    return prompt_draw(key).astype(jnp.bfloat16)


def draw_queries(key, part):
    normal_part = jax.random.normal(jax.random.fold_in(key, 23), (2, RESP, HEADS * HEAD_DIM), jnp.float32)
    result = jnp.clip(normal_part, -6.0, 6.0)
    return result.astype(jnp.bfloat16)


def draw_lengths(key, part):
    shorter = jax.random.randint(jax.random.fold_in(key, 41), (), RESP // 4, RESP + 1).astype(jnp.int32)
    longer = jnp.full((), RESP, jnp.int32)
    which = jax.random.randint(jax.random.fold_in(key, 43), (), 0, 2)
    return jnp.where(which == 0, jnp.stack([longer, shorter]), jnp.stack([shorter, longer])).astype(jnp.int32)


def level_of(key, dims, pieces, least, high):
    level, own = 1.0, jax.random.fold_in(key, 6)
    for position, shards_of in pieces:
        draws = jnp.exp(jax.random.uniform(jax.random.fold_in(own, position), (shards_of,), jnp.float32, least / len(pieces), high / len(pieces)))
        level = level * jnp.repeat(draws, dims[position] // shards_of).reshape([-1 if axis == position else 1 for axis in range(len(dims))])
    return level


def bell_draw(own_key, shape, deviation, limit, cuts=(), kind=jnp.bfloat16):
    values = jax.random.normal(own_key, shape, jnp.float32) * deviation
    if len(cuts) > 0:
        values = level_of(own_key, shape, cuts, -0.22, 0.18) * values
    return jnp.clip(values, min=-limit, max=limit).astype(kind)


def setup_inputs(seed: int = 0, part: int = 0) -> dict:
    arg_keys = jax.random.split(jax.random.key(seed), 8)
    own_keys = jax.random.split(jax.random.fold_in(arg_keys[7], part), 8)
    return {
        "prompt_keys": draw_prompt_keys(jax.random.fold_in(jax.random.fold_in(arg_keys[7], part), 71), part),
        "prompt_values": bell_draw(own_keys[1], (PROMPT, KV_HEADS * HEAD_DIM), 1.0, 6.0, ((0, 16),)),
        "queries": draw_queries(jax.random.fold_in(jax.random.fold_in(arg_keys[7], part), 71), part),
        "resp_keys": bell_draw(own_keys[3], (2, RESP, KV_HEADS * HEAD_DIM), 1.0, 6.0, ((1, 16),)),
        "resp_values": bell_draw(own_keys[4], (2, RESP, KV_HEADS * HEAD_DIM), 1.0, 6.0, ((1, 16),)),
        "cotangent": jnp.clip(jax.random.uniform(own_keys[5], (2, RESP, HEADS * HEAD_DIM), jnp.float32, -48.0, 48.0) * level_of(own_keys[5], (2, RESP, HEADS * HEAD_DIM), ((1, 16),), -0.4, 0.0), -48.0, 48.0).astype(jnp.bfloat16),
        "lengths": draw_lengths(jax.random.fold_in(jax.random.fold_in(arg_keys[7], part), 71), part),
    }


def rounded(array):
    return lax.optimization_barrier(array.astype(jnp.bfloat16)).astype(jnp.float32)


def one_branch(query_rows, cotangent_rows, key_rows, value_rows, length):
    group_size = HEADS // KV_HEADS
    score_scale = HEAD_DIM ** -0.5
    total_keys = key_rows.shape[0]
    keys_all = key_rows.reshape(total_keys, KV_HEADS, HEAD_DIM).astype(jnp.float32)
    values_all = value_rows.reshape(total_keys, KV_HEADS, HEAD_DIM).astype(jnp.float32)
    key_positions = jnp.arange(total_keys, dtype=jnp.int32) - PROMPT
    height = math.gcd(RESP, 256)
    number = RESP // height
    query_blocks = query_rows.reshape(number, height, KV_HEADS, group_size, HEAD_DIM)
    cotangent_blocks = cotangent_rows.reshape(number, height, KV_HEADS, group_size, HEAD_DIM)

    def advance(carried, element):
        key_sum, value_sum = carried
        queries, upstream, block_index = element
        positions = block_index * height + jnp.arange(height, dtype=jnp.int32)
        live_rows = positions < length
        queries = queries.astype(jnp.float32)
        upstream = jnp.where(live_rows[:, None, None, None], upstream.astype(jnp.float32), 0.0)
        scores = jnp.einsum("qkgd,nkd->kgqn", queries, keys_all) * score_scale
        scores = jnp.where(key_positions[None, :] <= positions[:, None], scores, -jnp.inf)
        log_norm = jax.nn.logsumexp(scores, axis=-1)
        probs = jnp.exp(scores - log_norm[..., None])
        probs_low = rounded(probs)
        attended = jnp.einsum("kgqn,nkd->kgqd", probs_low, values_all)
        attended = rounded(jnp.where(live_rows[None, None, :, None], attended, 0.0))
        delta = jnp.einsum("qkgd,kgqd->kgq", upstream, attended)
        prob_grad = jnp.einsum("qkgd,nkd->kgqn", upstream, values_all)
        score_grad = rounded(probs * (prob_grad - delta[..., None]))
        query_grad = jnp.einsum("kgqn,nkd->qkgd", score_grad, keys_all) * score_scale
        key_sum = key_sum + jnp.einsum("kgqn,qkgd->nkd", score_grad, queries) * score_scale
        value_sum = value_sum + jnp.einsum("kgqn,qkgd->nkd", probs_low, upstream)
        return (key_sum, value_sum), query_grad.reshape(height, HEADS * HEAD_DIM)

    empty_sum = jnp.zeros((total_keys, KV_HEADS, HEAD_DIM), jnp.float32)
    indices = jnp.arange(number, dtype=jnp.int32)
    (key_sum, value_sum), query_grads = lax.scan(advance, (empty_sum, empty_sum), (query_blocks, cotangent_blocks, indices))
    width = KV_HEADS * HEAD_DIM
    return query_grads.reshape(RESP, HEADS * HEAD_DIM), key_sum.reshape(total_keys, width), value_sum.reshape(total_keys, width)


def reference(prompt_keys, prompt_values, queries, resp_keys, resp_values, cotangent, lengths):
    query_grads = []
    resp_key_grads = []
    resp_value_grads = []
    prompt_key_sum = jnp.zeros(prompt_keys.shape, jnp.float32)
    prompt_value_sum = jnp.zeros(prompt_values.shape, jnp.float32)
    for branch in range(2):
        key_rows = jnp.concatenate([prompt_keys, resp_keys[branch]], axis=0)
        value_rows = jnp.concatenate([prompt_values, resp_values[branch]], axis=0)
        grad_rows, key_grad, value_grad = one_branch(queries[branch], cotangent[branch], key_rows, value_rows, lengths[branch])
        query_grads.append(grad_rows)
        prompt_key_sum = prompt_key_sum + key_grad[:PROMPT]
        prompt_value_sum = prompt_value_sum + value_grad[:PROMPT]
        resp_key_grads.append(key_grad[PROMPT:])
        resp_value_grads.append(value_grad[PROMPT:])
    return (jnp.stack(query_grads), jnp.stack(resp_key_grads), jnp.stack(resp_value_grads), prompt_key_sum, prompt_value_sum)
```

```python
import functools

import jax
import jax.numpy as jnp
from jax import lax
from jax.experimental import pallas as pl
from jax.experimental.pallas import tpu as pltpu
from jax.sharding import PartitionSpec as P

HEAD_DIM = 128
SCALE = HEAD_DIM ** (-0.5)
LOG2E = 1.4426950408889634
MIB = 1024 * 1024
RELAYED = 3


def remote(src, dst, send, recv, device):
    return pltpu.make_async_remote_copy(
        src_ref=src,
        dst_ref=dst,
        send_sem=send,
        recv_sem=recv,
        device_id={"ctx": device},
        device_id_type=pl.DeviceIdType.MESH,
    )


def offsets(groups, signs):
    order = [3] + list(range(4, groups)) + [1, 2]
    return [sign * far for far in order if far < groups for sign in signs]


def fused_kernel(
    groups, block, lengths, pk, pv, rk, rv, q, u,
    gq, grk, grv, gpk, gpv,
    kp, kr, kpos, qh, uh, qs, us, s_buf, d_buf, qt_buf, m_buf, l_buf, e_buf,
    tp, tr, xp, xr, sp, sr, rp, rr, lp, lr, fp, fr, dq,
    ysend, yrecv, ylocal, asend, arecv, bsend, dsend, drecv,
    csend, crecv, zsend, zrecv, lrecv, fsend, frecv, flocal,
    qsend, qrecv, qlocal, gsend, grecv, glocal,
):
    me = lax.axis_index("ctx")
    core, side, group = me % 2, (me // 2) % 2, me // 4

    def device(where, y, c):
        return where * 4 + y * 2 + c

    partner = device(group, side, 1 - core)
    across = device(group, 1 - side, core)
    prows, rrows = pk.shape[0], rk.shape[1]
    heads = kp.shape[1]
    wide = q.shape[2] // 2
    span = wide // heads
    members = span // HEAD_DIM
    inputs = ((pk, rk), (pv, rv))
    outputs = ((gpk, grk), (gpv, grv))
    parts = (0, 1, 2)
    pending = []

    def size_of(part):
        return prows if part == 0 else rrows

    def signs_out(part):
        return (1, -1) if part == 0 else (1,)

    def signs_back(part):
        return (-1, 1) if part == 0 else (-1,)

    def at_row(start, size):
        return pl.ds(pl.multiple_of(start, 16), size)

    def block_rows(part, c, where):
        size = 2 * size_of(part)
        return at_row(c * groups * size + where * size, size)

    def half_rows(part, where):
        size = 2 * size_of(part)
        return at_row(where * size, size)

    def own_rows(part):
        size = size_of(part)
        return at_row(core * groups * 2 * size + group * 2 * size + side * size, size)

    def pick(pair, k, part):
        return pair[0].at[:, k] if part == 0 else pair[1].at[:, k, part - 1]

    def stack(pair, k, part):
        return pair[0].at[k] if part == 0 else pair[1].at[k, part - 1]

    def head_columns(y, k):
        return pl.ds(pl.multiple_of((y * heads + k) * HEAD_DIM, HEAD_DIM), HEAD_DIM)

    def given(kind, part, cols):
        ref = inputs[kind][min(part, 1)]
        return ref.at[:, cols] if part == 0 else ref.at[part - 1, :, cols]

    def valid(where):
        return jnp.logical_and(where >= 0, where < groups)

    def later(cond, copy):
        pending.append((cond, copy))

    units = [(k, b) for k in range(heads) for b in range(2)]
    order = [(k, part) for k in range(heads) for part in parts]

    stays = {}
    for k, part in order:
        for kind in range(2):
            dst = pick((kp, kr), k, part).at[kind, own_rows(part), :]
            stay = pltpu.make_async_copy(
                given(kind, part, head_columns(side, k)), dst, ylocal.at[part, k, kind]
            )
            stay.start()
            stays[k, part, kind] = stay
    query_stays = {}
    for k, b in units:
        cols = pl.ds(pl.multiple_of((side * heads + k) * span, span), span)
        for i, (src, dst) in enumerate(((q, qh), (u, uh))):
            stay = pltpu.make_async_copy(
                src.at[b, :, cols], dst.at[side, b, :, pl.ds(k * span, span)], qlocal.at[i, k, b]
            )
            stay.start()
            query_stays[i, k, b] = stay

    for c in range(2):
        for where in range(groups):
            @pl.when(where > group)
            def _(c=c, where=where):
                empty = jnp.zeros((2, heads, 2, 2 * rrows, HEAD_DIM), kr.dtype)
                kr[:, :, :, pl.ds((c * groups + where) * 2 * rrows, 2 * rrows), :] = empty
            for y in range(2):
                start = ((c * groups + where) * 2 + y) * rrows
                kpos[pl.ds(start, rrows), :] = device(where, y, c) * rrows + lax.broadcasted_iota(
                    jnp.int32, (rrows, 1), 0
                )
    for ref in (rp, rr, lp, lr):
        ref[...] = jnp.zeros_like(ref)

    barrier = pltpu.get_barrier_semaphore()
    peers = [partner, across] + [device((group + i) % groups, side, core) for i in range(1, groups)]
    for other in peers:
        pl.semaphore_signal(
            barrier, inc=1, device_id={"ctx": other}, device_id_type=pl.DeviceIdType.MESH
        )
    pl.semaphore_wait(barrier, len(peers))

    crossing = {}
    for k, part in order:
        for kind in range(2):
            dst = pick((kp, kr), k, part).at[kind, own_rows(part), :]
            away = remote(
                given(kind, part, head_columns(1 - side, k)), dst,
                ysend.at[part, k, kind], yrecv.at[part, k, kind], across,
            )
            away.start()
            crossing[k, part, kind] = away
            later(None, away)
    query_moves = {}
    for k, b in units:
        cols = pl.ds(pl.multiple_of(((1 - side) * heads + k) * span, span), span)
        for i, (src, dst) in enumerate(((q, qh), (u, uh))):
            away = remote(
                src.at[b, :, cols], dst.at[side, b, :, pl.ds(k * span, span)],
                qsend.at[i, k, b], qrecv.at[i, k, b], across,
            )
            away.start()
            query_moves[i, k, b] = away
            later(None, away)

    def shared(k, part, where):
        ref = pick((kp, kr), k, part).at[:, block_rows(part, core, where), :]
        return remote(ref, ref, dsend.at[part, k, where], drecv.at[part, k, where], partner)

    def fan(k, part):
        for kind in range(2):
            crossing[k, part, kind].wait_recv()
            stays[k, part, kind].wait()
        ref = pick((kp, kr), k, part).at[:, block_rows(part, core, group), :]
        near = shared(k, part, group)
        near.start()
        later(None, near)
        for i, delta in enumerate(offsets(groups, signs_out(part))):
            if abs(delta) == RELAYED:
                continue
            to = group + delta
            copy = remote(
                ref, ref, asend.at[part, k, i], arecv.at[part, k, group], device(to, side, core)
            )
            pl.when(valid(to))(copy.start)
            later(valid(to), copy)

    def arrive(k, part, delta):
        origin = group - delta
        step = 1 if delta > 0 else -1
        ref = pick((kp, kr), k, part).at[:, block_rows(part, core, origin), :]
        copy = remote(ref, ref, asend.at[part, k, 0], arecv.at[part, k, origin], partner)
        near = shared(k, part, origin)

        @pl.when(valid(origin))
        def _():
            copy.wait_recv()
            near.start()

        later(valid(origin), near)
        if abs(delta) == RELAYED - 1:
            go = jnp.logical_and(valid(origin), valid(group + step))
            copy = remote(
                ref, ref, bsend.at[part, k, 0 if step > 0 else 1], arecv.at[part, k, origin],
                device(group + step, side, core),
            )
            pl.when(go)(copy.start)
            later(go, copy)

    def arrivals(k, part):
        near_first = sorted(offsets(groups, signs_out(part)), key=abs)
        return [(k, part, delta) for delta in near_first]

    def gathered(k, part):
        shared(k, part, group).wait_recv()
        for delta in offsets(groups, signs_out(part)):
            origin = group - delta
            pl.when(valid(origin))(shared(k, part, origin).wait_recv)

    def meet(k, part):
        rows = block_rows(part, 1 - core, 0)
        size = groups * 2 * size_of(part)
        rows = at_row((1 - core) * size, size)
        copy = remote(
            pick((tp, tr), k, part).at[:, rows, :], pick((xp, xr), k, part),
            csend.at[part, k], crecv.at[part, k], partner,
        )
        copy.start()
        later(None, copy)
        met[k, part] = copy

    met = {}

    def total(kind, k, part, where):
        mine = pick((tp, tr), k, part).at[kind, block_rows(part, core, where), :]
        other = pick((xp, xr), k, part).at[kind, half_rows(part, where), :]
        return mine[...] + other[...]

    def push(k, part, fars):
        signs = signs_back(part)
        for i, delta in enumerate(offsets(groups, signs)):
            if abs(delta) not in fars:
                continue
            step = 1 if delta > 0 else -1
            way = 0 if step < 0 else 1
            to = group + delta
            out = stack((sp, sr), k, part).at[i]
            passing = stack((lp, lr), k, part).at[way]
            relayed = abs(delta) == RELAYED
            gathers = abs(delta) == RELAYED - 1
            if relayed:
                dst, recv, where = passing, lrecv.at[part, k, way], group + step
            else:
                dst = stack((rp, rr), k, part).at[group]
                recv, where = zrecv.at[part, k, group], to
            copy = remote(out, dst, zsend.at[part, k, i], recv, device(where, side, core))
            if gathers:
                wait = remote(out, passing, zsend.at[part, k, i], lrecv.at[part, k, way], partner)
                pl.when(jnp.logical_and(valid(to), valid(group - step)))(wait.wait_recv)

            @pl.when(valid(to))
            def _(delta=delta, to=to, out=out, passing=passing, gathers=gathers, copy=copy):
                for kind in range(2):
                    value = total(kind, k, part, to)
                    if gathers:
                        value = value + passing[kind].astype(jnp.float32)
                    out[kind] = value.astype(jnp.bfloat16)
                copy.start()

            later(valid(to), copy)

    def finish(k, part):
        got = stack((rp, rr), k, part)
        final = stack((fp, fr), k, part)
        for delta in offsets(groups, signs_back(part)):
            if abs(delta) == RELAYED:
                continue
            origin = group - delta
            slot = got.at[origin]
            copy = remote(slot, slot, zsend.at[part, k, 0], zrecv.at[part, k, origin], partner)
            pl.when(valid(origin))(copy.wait_recv)
        for kind in range(2):
            value = total(kind, k, part, group)
            for origin in range(groups):
                value = value + got[origin, kind].astype(jnp.float32)
            final[kind] = value.astype(jnp.bfloat16)
            out = outputs[kind][min(part, 1)]
            cols = head_columns(side, k)
            dst = out.at[:, cols] if part == 0 else out.at[part - 1, :, cols]
            size = size_of(part)
            away = remote(
                final.at[kind, at_row((1 - side) * size, size), :], dst,
                fsend.at[part, k, kind], frecv.at[part, k, kind], across,
            )
            away.start()
            stay = pltpu.make_async_copy(
                final.at[kind, at_row(side * size, size), :], dst, flocal.at[part, k, kind]
            )
            stay.start()
            outgoing.extend((away, stay))

    outgoing = []
    half = members * rrows
    lanes = 2 * half
    prompt_blocks = kp.shape[2] // block
    resp_blocks = kr.shape[3] // block
    factor = SCALE * LOG2E
    lane = lax.broadcasted_iota(jnp.int32, (1, lanes), 1)
    row_of = lax.rem(lane, rrows)
    first_row = device(group, 0, core) * rrows
    positions = first_row + row_of + jnp.where(lane < half, 0, 2 * rrows)
    row_iota = lax.broadcasted_iota(jnp.int32, (rrows, 1), 0)
    nt = (((1,), (1,)), ((), ()))

    def key_rows(j):
        return pl.ds(pl.multiple_of(j * block, block), block)

    def compute(unit, ticks):
        k, b = units[unit]
        length = lengths[b]
        for source in range(2):
            live = first_row + source * 2 * rrows + row_iota < length
            for g in range(members):
                cols = pl.ds((k * members + g) * HEAD_DIM, HEAD_DIM)
                at = pl.ds(source * half + g * rrows, rrows)
                qs[at, :] = qh[source, b, :, cols]
                rows = uh[source, b, :, cols]
                us[at, :] = jnp.where(live, rows, jnp.zeros_like(rows))
        m_buf[...] = jnp.full_like(m_buf, -jnp.inf)
        l_buf[...] = jnp.zeros_like(l_buf)
        e_buf[...] = jnp.zeros_like(e_buf)
        qt_buf[...] = jnp.zeros_like(qt_buf)
        ticks(0)

        def scores(keys, at, j, causal):
            s = lax.dot_general(keys, qs[...], nt, preferred_element_type=jnp.float32)
            if causal:
                s = jnp.where(kpos[key_rows(j), :] <= positions, s, -jnp.inf)
            s_buf[at, :] = s
            m_buf[...] = jnp.maximum(m_buf[...], jnp.max(s, axis=0, keepdims=True))

        @pl.loop(0, prompt_blocks, unroll=True)
        def _(j):
            scores(kp[0, k, key_rows(j), :], key_rows(j), j, False)

        ticks(1)

        @pl.loop(0, resp_blocks, unroll=True)
        def _(j):
            scores(kr[0, k, b, key_rows(j), :], key_rows(prompt_blocks + j), j, True)

        ticks(2)
        shift = m_buf[...] * factor

        def weights(vals, at):
            p = jnp.exp2(s_buf[at, :] * factor - shift)
            d = lax.dot_general(vals, us[...], nt, preferred_element_type=jnp.float32)
            l_buf[...] += jnp.sum(p, axis=0, keepdims=True)
            e_buf[...] += jnp.sum(p * d, axis=0, keepdims=True)
            s_buf[at, :] = p
            d_buf[at, :] = d

        @pl.loop(0, prompt_blocks, unroll=True)
        def _(j):
            weights(kp[1, k, key_rows(j), :], key_rows(j))

        ticks(3)

        @pl.loop(0, resp_blocks, unroll=True)
        def _(j):
            weights(kr[1, k, b, key_rows(j), :], key_rows(prompt_blocks + j))

        ticks(4)
        inverse = 1.0 / l_buf[...]
        delta = e_buf[...] * inverse

        def grads(keys, at):
            p = s_buf[at, :] * inverse
            ds = (p * (d_buf[at, :] - delta)).astype(jnp.bfloat16)
            dv = jnp.dot(p.astype(jnp.bfloat16), us[...], preferred_element_type=jnp.float32)
            dk = jnp.dot(ds, qs[...], preferred_element_type=jnp.float32) * SCALE
            qt_buf[...] += jnp.dot(keys.T, ds, preferred_element_type=jnp.float32)
            return dk, dv

        @pl.loop(0, prompt_blocks, unroll=True)
        def _(j):
            at = key_rows(j)
            pair = grads(kp[0, k, at, :], at)
            for kind in range(2):
                if b == 0:
                    tp[kind, k, at, :] = pair[kind]
                else:
                    tp[kind, k, at, :] += pair[kind]

        ticks(5)

        @pl.loop(0, resp_blocks, unroll=True)
        def _(j):
            at = key_rows(j)
            pair = grads(kr[0, k, b, at, :], key_rows(prompt_blocks + j))
            for kind in range(2):
                tr[kind, k, b, at, :] = pair[kind]

        ticks(6)
        result = (qt_buf[...].T * SCALE).astype(jnp.bfloat16)
        for source in range(2):
            for g in range(members):
                start = source * half + g * rrows
                dq[source, b, :, pl.ds((k * members + g) * HEAD_DIM, HEAD_DIM)] = result[
                    start : start + rrows
                ]
        cols = pl.ds(k * span, span)
        to = pl.ds(pl.multiple_of((side * heads + k) * span, span), span)
        away = remote(
            dq.at[1 - side, b, :, cols], gq.at[b, :, to], gsend.at[k, b], grecv.at[k, b], across
        )
        away.start()
        stay = pltpu.make_async_copy(dq.at[side, b, :, cols], gq.at[b, :, to], glocal.at[k, b])
        stay.start()
        outgoing.extend((away, stay))

    def needs(unit):
        k, b = units[unit]
        return [(k, 0), (k, 1)] if b == 0 else [(k, 2)]

    def yields(unit):
        k, b = units[unit]
        return [(k, 1)] if b == 0 else [(k, 0), (k, 2)]

    fars = sorted({abs(delta) for delta in offsets(groups, (1,))})
    early = tuple(far for far in fars if far != RELAYED - 1)
    late = tuple(far for far in fars if far == RELAYED - 1)

    for k, part in order:
        fan(k, part)
    for k, part in needs(0):
        for item in arrivals(k, part):
            arrive(*item)
    for k, part in needs(0):
        gathered(k, part)

    last = len(units) - 1
    for unit in range(last + 1):
        k, b = units[unit]
        for i in range(2):
            query_stays[i, k, b].wait()
            query_moves[i, k, b].wait_recv()

        def ticks(at, unit=unit, k=k, b=b):
            if unit < last:
                if at == 4:
                    for pair in needs(unit + 1):
                        for item in arrivals(*pair):
                            arrive(*item)
            if unit > 0:
                if at == 1:
                    for pair in yields(unit - 1):
                        met[pair].wait_recv()
                        push(*pair, early)
                if at == 3:
                    for pair in yields(unit - 1):
                        push(*pair, late)
            if unit > 1 and at == 2:
                for pair in yields(unit - 2):
                    finish(*pair)
            if at == 5 and b == 1:
                meet(k, 0)
            if at == 6:
                meet(k, b + 1)

        compute(unit, ticks)
        if unit < last:
            for pair in needs(unit + 1):
                gathered(*pair)
    for pair in yields(last):
        met[pair].wait_recv()
        push(*pair, early)
    for pair in yields(last):
        push(*pair, late)
    for pair in yields(last - 1) + yields(last):
        finish(*pair)
    for cond, copy in pending:
        if cond is None:
            copy.wait_send()
        else:
            pl.when(cond)(copy.wait_send)
    for copy in outgoing:
        copy.wait()


def key_block(prompt, resp):
    size = 256
    while prompt % size or resp % size:
        size //= 2
    return size


def settle_kernel(*refs):
    count = (len(refs) - 2) // 4
    sources, targets = refs[:count], refs[count : 2 * count]
    holds, wides = refs[2 * count : 3 * count], refs[3 * count : 4 * count]
    taken, given = refs[4 * count :]
    pieces = []
    for i, (source, target, hold, wide) in enumerate(zip(sources, targets, holds, wides)):
        chunks = 4 if source.size > 1 << 18 else 1
        step = source.shape[-1] // chunks
        for c in range(chunks):
            cut = (slice(None),) * (len(source.shape) - 1) + (pl.ds(c * step, step),)
            taking = pltpu.make_async_copy(source.at[cut], hold.at[cut], taken.at[i, c])
            taking.start()
            giving = pltpu.make_async_copy(wide.at[cut], target.at[cut], given.at[i, c])
            pieces.append((taking, giving, hold, wide, cut))
    for taking, giving, hold, wide, cut in pieces:
        taking.wait()
        wide[cut] = hold[cut].astype(wide.dtype)
        giving.start()
    for piece in pieces:
        piece[1].wait()


def settle(*arrays):
    hbm = pl.BlockSpec(memory_space=pl.ANY)
    dma = pltpu.SemaphoreType.DMA
    return pl.pallas_call(
        settle_kernel,
        out_shape=tuple(jax.ShapeDtypeStruct(x.shape, jnp.float32) for x in arrays),
        in_specs=[hbm] * len(arrays),
        out_specs=(hbm,) * len(arrays),
        scratch_shapes=[pltpu.VMEM(x.shape, x.dtype) for x in arrays]
        + [pltpu.VMEM(x.shape, jnp.float32) for x in arrays]
        + [dma((len(arrays), 4)), dma((len(arrays), 4))],
        compiler_params=pltpu.CompilerParams(vmem_limit_bytes=60 * MIB),
        name="settle",
    )(*arrays)


def local(prompt_keys, prompt_values, queries, resp_keys, resp_values, cotangent, lengths):
    devices = lax.axis_size("ctx")
    groups = devices // 4
    prows, columns = prompt_keys.shape
    rows, wide = queries.shape[1], queries.shape[2] // 2
    heads = columns // 2 // HEAD_DIM
    prompt, resp = prows * devices, rows * devices
    smem = pl.BlockSpec(memory_space=pltpu.SMEM)
    hbm = pl.BlockSpec(memory_space=pl.ANY)
    shape = jax.ShapeDtypeStruct
    bf16, f32 = jnp.bfloat16, jnp.float32
    vmem, dma = pltpu.VMEM, pltpu.SemaphoreType.DMA
    block = key_block(prompt, resp)
    lanes = 2 * rows * (wide // HEAD_DIM) // heads
    total = prompt + resp
    both, one = len(offsets(groups, (1, -1))), len(offsets(groups, (1,)))
    outs = pl.pallas_call(
        functools.partial(fused_kernel, groups, block),
        out_shape=(
            shape((2, rows, 2 * wide), bf16),
            shape((2, rows, columns), bf16), shape((2, rows, columns), bf16),
            shape((prows, columns), bf16), shape((prows, columns), bf16),
        ),
        in_specs=[smem] + [hbm] * 6,
        out_specs=(hbm,) * 5,
        scratch_shapes=[
            vmem((2, heads, prompt, HEAD_DIM), bf16),
            vmem((2, heads, 2, resp, HEAD_DIM), bf16),
            vmem((resp, 1), jnp.int32),
            vmem((2, 2, rows, wide), bf16), vmem((2, 2, rows, wide), bf16),
            vmem((lanes, HEAD_DIM), bf16), vmem((lanes, HEAD_DIM), bf16),
            vmem((total, lanes), f32), vmem((total, lanes), f32),
            vmem((HEAD_DIM, lanes), f32),
            vmem((1, lanes), f32), vmem((1, lanes), f32), vmem((1, lanes), f32),
            vmem((2, heads, prompt, HEAD_DIM), f32),
            vmem((2, heads, 2, resp, HEAD_DIM), f32),
            vmem((2, heads, prompt // 2, HEAD_DIM), f32),
            vmem((2, heads, 2, resp // 2, HEAD_DIM), f32),
            vmem((heads, both, 2, 2 * prows, HEAD_DIM), bf16),
            vmem((heads, 2, one, 2, 2 * rows, HEAD_DIM), bf16),
            vmem((heads, groups, 2, 2 * prows, HEAD_DIM), bf16),
            vmem((heads, 2, groups, 2, 2 * rows, HEAD_DIM), bf16),
            vmem((heads, 2, 2, 2 * prows, HEAD_DIM), bf16),
            vmem((heads, 2, 1, 2, 2 * rows, HEAD_DIM), bf16),
            vmem((heads, 2, 2 * prows, HEAD_DIM), bf16),
            vmem((heads, 2, 2, 2 * rows, HEAD_DIM), bf16),
            vmem((2, 2, rows, wide), bf16),
            dma((3, heads, 2)), dma((3, heads, 2)), dma((3, heads, 2)),
            dma((3, heads, both)), dma((3, heads, groups)), dma((3, heads, 2)),
            dma((3, heads, groups)), dma((3, heads, groups)),
            dma((3, heads)), dma((3, heads)),
            dma((3, heads, both)), dma((3, heads, groups)), dma((3, heads, 2)),
            dma((3, heads, 2)), dma((3, heads, 2)), dma((3, heads, 2)),
            dma((2, heads, 2)), dma((2, heads, 2)), dma((2, heads, 2)),
            dma((heads, 2)), dma((heads, 2)), dma((heads, 2)),
        ],
        compiler_params=pltpu.CompilerParams(
            collective_id=0, has_side_effects=True, vmem_limit_bytes=60 * MIB
        ),
        name="fused",
    )(lengths, prompt_keys, prompt_values, resp_keys, resp_values, queries, cotangent)
    return settle(*outs)


def solution(mesh):
    placed = (
        P(("pairs", "ctx"), None),
        P(("pairs", "ctx"), None),
        P("pairs", "ctx", None),
        P("pairs", "ctx", None),
        P("pairs", "ctx", None),
        P("pairs", "ctx", None),
        P("pairs"),
    )
    return jax.shard_map(
        local,
        mesh=mesh,
        in_specs=placed,
        out_specs=(
            P("pairs", "ctx", None),
            P("pairs", "ctx", None),
            P("pairs", "ctx", None),
            P(("pairs", "ctx"), None),
            P(("pairs", "ctx"), None),
        ),
        check_vma=False,
    )
```

```python
import functools

import jax
import jax.numpy as jnp
from jax import lax
from jax.experimental import pallas as pl
from jax.experimental.pallas import tpu as pltpu
from jax.sharding import PartitionSpec as P

HEAD_DIM = 128
SCALE = HEAD_DIM ** (-0.5)
LOG2E = 1.4426950408889634
MIB = 1024 * 1024
RELAYED = 3


def remote(src, dst, send, recv, device):
    return pltpu.make_async_remote_copy(
        src_ref=src,
        dst_ref=dst,
        send_sem=send,
        recv_sem=recv,
        device_id={"ctx": device},
        device_id_type=pl.DeviceIdType.MESH,
    )


def offsets(groups, signs):
    order = [2, 1, 3] + list(range(4, groups))
    return [sign * far for far in order if far < groups for sign in signs]


def fused_kernel(
    groups, block, lengths, pk, pv, rk, rv, q, u,
    gq, grk, grv, gpk, gpv,
    kp, kr, bp, br, kpos, quh, quf, qs, us, s_buf, d_buf, qt_buf, m_buf, l_buf, e_buf,
    tp, tr, xp, xr, sp, sr, rp, rr, fb, dq,
    local_sem, ysend, yrecv, qsend, qrecv, asend_p, asend_r, arecv, bsend, dsend, drecv,
    csend, crecv, zsend_p, zsend_r, zrecv, fsem, gsem,
):
    me = lax.axis_index("ctx")
    core, side, group = me % 2, (me // 2) % 2, me // 4

    def device(where, y, c):
        return where * 4 + y * 2 + c

    partner = device(group, side, 1 - core)
    across = device(group, 1 - side, core)
    prows, rrows = pk.shape[0], rk.shape[1]
    heads = kp.shape[1]
    wide = q.shape[2] // 2
    span = wide // heads
    members = span // HEAD_DIM
    inputs = ((pk, rk), (pv, rv))
    outputs = ((gpk, grk), (gpv, grv))
    parts = (0, 1, 2)

    def size_of(part):
        return prows if part == 0 else rrows

    def signs_out(part):
        return (1, -1) if part == 0 else (1,)

    def signs_back(part):
        return (-1, 1) if part == 0 else (-1,)

    def at_row(start, size):
        return pl.ds(pl.multiple_of(start, 16), size)

    def block_rows(part, c, where):
        size = 2 * size_of(part)
        return at_row(c * groups * size + where * size, size)

    def side_rows(part, y):
        size = size_of(part)
        return at_row(core * groups * 2 * size + group * 2 * size + y * size, size)

    def half_rows(part, where):
        size = 2 * size_of(part)
        return at_row(where * size, size)

    def core_rows(part, c):
        size = groups * 2 * size_of(part)
        return at_row(c * size, size)

    def pick(pair, k, part):
        return pair[0].at[:, k] if part == 0 else pair[1].at[:, k, part - 1]

    def stack(pair, k, part):
        return pair[0].at[k] if part == 0 else pair[1].at[k, part - 1]

    def head_columns(y, k):
        return pl.ds(pl.multiple_of((y * heads + k) * HEAD_DIM, HEAD_DIM), HEAD_DIM)

    def query_columns(y, k):
        return pl.ds(pl.multiple_of((y * heads + k) * span, span), span)

    def given(kind, part, cols):
        ref = inputs[kind][min(part, 1)]
        return ref.at[:, cols] if part == 0 else ref.at[part - 1, :, cols]

    def valid(where):
        return jnp.logical_and(where >= 0, where < groups)

    def relays(k, delta):
        return k == 0 and abs(delta) == RELAYED

    units = [(k, b) for k in range(heads) for b in range(2)]
    order = [(k, part) for k in range(heads) for part in parts]

    for c in range(2):
        for where in range(groups):
            @pl.when(where > group)
            def _(c=c, where=where):
                empty = jnp.zeros((2, heads, 2, 2 * rrows, HEAD_DIM), kr.dtype)
                kr[:, :, :, pl.ds((c * groups + where) * 2 * rrows, 2 * rrows), :] = empty
    for ref in (rp, rr):
        ref[...] = jnp.zeros_like(ref)

    barrier = pltpu.get_barrier_semaphore()
    peers = [partner, across] + [device((group + i) % groups, side, core) for i in range(1, groups)]
    for other in peers:
        pl.semaphore_signal(
            barrier, inc=1, device_id={"ctx": other}, device_id_type=pl.DeviceIdType.MESH
        )

    for k, part in order:
        for kind in range(2):
            pltpu.make_async_copy(
                given(kind, part, head_columns(1 - side, k)),
                stack((bp, br), k, part).at[kind], local_sem.at[min(part, 1)],
            ).start()
            pltpu.make_async_copy(
                given(kind, part, head_columns(side, k)),
                pick((kp, kr), k, part).at[kind, side_rows(part, side), :],
                local_sem.at[2 + min(part, 1)],
            ).start()
    wide_own = pl.ds(pl.multiple_of(side * wide, wide), wide)
    wide_far = pl.ds(pl.multiple_of((1 - side) * wide, wide), wide)
    for i, src in enumerate((q, u)):
        pltpu.make_async_copy(src.at[:, :, wide_far], quf.at[i], local_sem.at[4]).start()
        pltpu.make_async_copy(src.at[:, :, wide_own], quh.at[i, side], local_sem.at[5]).start()

    for c in range(2):
        for where in range(groups):
            for y in range(2):
                start = ((c * groups + where) * 2 + y) * rrows
                kpos[pl.ds(start, rrows), :] = device(where, y, c) * rrows + lax.broadcasted_iota(
                    jnp.int32, (rrows, 1), 0
                )

    def landed(ref, i):
        pltpu.make_async_copy(ref, ref, local_sem.at[i]).wait()

    def hello():
        pl.semaphore_wait(barrier, len(peers))

    hello()
    landed(bp, 0)
    landed(br, 1)

    def crossing(k, part, y):
        ref = pick((kp, kr), k, part).at[:, side_rows(part, y), :]
        return remote(ref, ref, ysend.at[min(part, 1)], yrecv.at[part, k], across)

    def cross(k, part):
        for kind in range(2):
            remote(
                stack((bp, br), k, part).at[kind],
                pick((kp, kr), k, part).at[kind, side_rows(part, side), :],
                ysend.at[min(part, 1)], yrecv.at[part, k], across,
            ).start()

    def query_crossing(k, b, y):
        ref = quh.at[:, y, b, :, pl.ds(k * span, span)]
        return remote(ref, ref, qsend.at[0], qrecv.at[k, b], across)

    def query_cross(k, b):
        cols = pl.ds(k * span, span)
        for i in range(2):
            remote(
                quf.at[i, b, :, cols], quh.at[i, side, b, :, cols],
                qsend.at[0], qrecv.at[k, b], across,
            ).start()

    def shared(k, part):
        ref = pick((kp, kr), k, part).at[:, core_rows(part, core), :]
        return remote(ref, ref, dsend.at[min(part, 1)], drecv.at[part, k], partner)

    def fanned(k, part, i):
        return asend_p.at[k, i] if part == 0 else asend_r.at[k, i]

    def fan(k, part):
        crossing(k, part, 1 - side).wait_recv()
        ref = pick((kp, kr), k, part).at[:, block_rows(part, core, group), :]
        for i, delta in enumerate(offsets(groups, signs_out(part))):
            if relays(k, delta):
                continue
            to = group + delta
            copy = remote(
                ref, ref, fanned(k, part, i), arecv.at[part, k, group], device(to, side, core)
            )
            pl.when(valid(to))(copy.start)

    def arrive(k, part):
        for delta in sorted(offsets(groups, signs_out(part)), key=abs):
            origin = group - delta
            step = 1 if delta > 0 else -1
            ref = pick((kp, kr), k, part).at[:, block_rows(part, core, origin), :]
            copy = remote(ref, ref, bsend.at[0], arecv.at[part, k, origin], partner)
            pl.when(valid(origin))(copy.wait_recv)
            if k == 0 and abs(delta) == RELAYED - 1:
                copy = remote(
                    ref, ref, bsend.at[2 if part > 0 else (1 - step) // 2],
                    arecv.at[part, k, origin], device(group + step, side, core),
                )
                pl.when(jnp.logical_and(valid(origin), valid(group + step)))(copy.start)
        shared(k, part).start()

    def met(k, part):
        ref = pick((tp, tr), k, part).at[:, core_rows(part, 1 - core), :]
        return remote(
            ref, pick((xp, xr), k, part), csend.at[min(part, 1)], crecv.at[part, k], partner
        )

    def meet(k, part):
        met(k, part).start()

    def total(kind, k, part, where):
        mine = pick((tp, tr), k, part).at[kind, block_rows(part, core, where), :]
        other = pick((xp, xr), k, part).at[kind, half_rows(part, where), :]
        return mine[...] + other[...]

    def returns(part):
        return offsets(groups, signs_back(part)) + [0]

    def returned(part, i):
        return zsend_p.at[i] if part == 0 else zsend_r.at[i]

    def push(k, part):
        met(k, part).wait_recv()
        size = size_of(part)
        for i, delta in enumerate(returns(part)):
            to = group + delta
            out = stack((sp, sr), k, part).at[i]
            sides = range(2) if delta else (1 - side,)
            copies = [
                remote(
                    out.at[y], stack((rp, rr), k, part).at[side, group], returned(part, i),
                    zrecv.at[part, k, group], device(to, y, core),
                )
                for y in sides
            ]

            @pl.when(valid(to))
            def _(to=to, out=out, copies=copies):
                for kind in range(2):
                    value = total(kind, k, part, to).astype(jnp.bfloat16)
                    for y in range(2):
                        out[y, kind] = value[y * size : (y + 1) * size]
                for copy in copies:
                    copy.start()

    starts = (0, prows, prows + rrows)

    def finish(k, part):
        got = stack((rp, rr), k, part)
        size = size_of(part)
        for delta in returns(part):
            origin = group - delta
            slot = got.at[:, origin] if delta else got.at[0, origin]
            copy = remote(slot, slot, bsend.at[0], zrecv.at[part, k, origin], partner)
            pl.when(valid(origin))(copy.wait_recv)
        rows = pl.ds(starts[part], size)
        near = at_row(group * 2 * size + side * size, size)
        for kind in range(2):
            mine = pick((tp, tr), k, part).at[kind, side_rows(part, side), :]
            own = mine[...] + pick((xp, xr), k, part).at[kind, near, :][...]
            out = outputs[kind][min(part, 1)]
            for y in range(2):
                value = jnp.where(side == y, own, jnp.zeros_like(own))
                for origin in range(groups):
                    value = value + got[y, origin, kind].astype(jnp.float32)
                fb[k, kind, y, rows, :] = value
                cols = pl.ds((y * heads + k) * HEAD_DIM, HEAD_DIM)
                dst = out.at[:, cols] if part == 0 else out.at[part - 1, :, cols]
                pltpu.make_async_copy(fb.at[k, kind, y, rows, :], dst, fsem.at[0]).start()

    def drain():
        remote(bp, bp, ysend.at[0], ysend.at[0], across).wait_send()
        remote(br, br, ysend.at[1], ysend.at[1], across).wait_send()
        remote(quf, quf, qsend.at[0], qsend.at[0], across).wait_send()
        ref = kp.at[:, :, core_rows(0, core), :]
        remote(ref, ref, dsend.at[0], dsend.at[0], partner).wait_send()
        ref = kr.at[:, :, :, core_rows(1, core), :]
        remote(ref, ref, dsend.at[1], dsend.at[1], partner).wait_send()
        ref = tp.at[:, :, core_rows(0, 1 - core), :]
        remote(ref, ref, csend.at[0], csend.at[0], partner).wait_send()
        ref = tr.at[:, :, :, core_rows(1, 1 - core), :]
        remote(ref, ref, csend.at[1], csend.at[1], partner).wait_send()
        for part in range(2):
            for i, delta in enumerate(offsets(groups, signs_out(part))):
                refs = []
                for k in range(heads):
                    if not relays(k, delta):
                        if part == 0:
                            ref = kp.at[:, k, block_rows(0, core, group), :]
                        else:
                            ref = kr.at[:, k, :, block_rows(1, core, group), :]
                        refs.append((ref, fanned(k, part, i)))

                @pl.when(valid(group + delta))
                def _(refs=refs):
                    for ref, sem in refs:
                        remote(ref, ref, sem, sem, across).wait_send()

                if abs(delta) == RELAYED - 1:
                    step = 1 if delta > 0 else -1
                    origin = group - delta
                    if part == 0:
                        ref = kp.at[:, 0, block_rows(0, core, origin), :]
                    else:
                        ref = kr.at[:, 0, :, block_rows(1, core, origin), :]
                    sem = bsend.at[2 if part > 0 else (1 - step) // 2]
                    pl.when(jnp.logical_and(valid(origin), valid(group + step)))(
                        remote(ref, ref, sem, sem, across).wait_send
                    )
            for i, delta in enumerate(returns(part)):
                ref = sp.at[:, i] if part == 0 else sr.at[:, :, i]
                if delta == 0:
                    ref = sp.at[:, i, 0] if part == 0 else sr.at[:, :, i, 0]
                sem = returned(part, i)
                pl.when(valid(group + delta))(remote(ref, ref, sem, sem, across).wait_send)

    def close():
        ref = dq.at[0]
        remote(ref, ref, gsem.at[0], gsem.at[1], across).wait()
        pltpu.make_async_copy(ref, ref, gsem.at[2]).wait()
        pltpu.make_async_copy(fb, fb, fsem.at[0]).wait()

    half = members * rrows
    lanes = 2 * half
    prompt_blocks = kp.shape[2] // block
    resp_blocks = kr.shape[3] // block
    factor = SCALE * LOG2E
    lane = lax.broadcasted_iota(jnp.int32, (1, lanes), 1)
    row_of = lax.rem(lane, rrows)
    first_row = device(group, 0, core) * rrows
    positions = first_row + row_of + jnp.where(lane < half, 0, 2 * rrows)
    row_iota = lax.broadcasted_iota(jnp.int32, (rrows, 1), 0)
    nt = (((1,), (1,)), ((), ()))

    def key_rows(j):
        return pl.ds(pl.multiple_of(j * block, block), block)

    def compute(unit, ticks):
        k, b = units[unit]
        length = lengths[b]
        for source in range(2):
            live = first_row + source * 2 * rrows + row_iota < length
            for g in range(members):
                cols = pl.ds((k * members + g) * HEAD_DIM, HEAD_DIM)
                at = pl.ds(source * half + g * rrows, rrows)
                qs[at, :] = quh[0, source, b, :, cols]
                rows = quh[1, source, b, :, cols]
                us[at, :] = jnp.where(live, rows, jnp.zeros_like(rows))
        m_buf[...] = jnp.full_like(m_buf, -jnp.inf)
        l_buf[...] = jnp.zeros_like(l_buf)
        e_buf[...] = jnp.zeros_like(e_buf)
        qt_buf[...] = jnp.zeros_like(qt_buf)
        ticks(0)

        def scores(keys, at, j, causal):
            s = lax.dot_general(keys, qs[...], nt, preferred_element_type=jnp.float32)
            if causal:
                s = jnp.where(kpos[key_rows(j), :] <= positions, s, -jnp.inf)
            s_buf[at, :] = s
            m_buf[...] = jnp.maximum(m_buf[...], jnp.max(s, axis=0, keepdims=True))

        @pl.loop(0, prompt_blocks, unroll=True)
        def _(j):
            scores(kp[0, k, key_rows(j), :], key_rows(j), j, False)

        ticks(1)

        @pl.loop(0, resp_blocks, unroll=True)
        def _(j):
            scores(kr[0, k, b, key_rows(j), :], key_rows(prompt_blocks + j), j, True)

        ticks(2)
        shift = m_buf[...] * factor

        def weights(vals, at):
            p = jnp.exp2(s_buf[at, :] * factor - shift)
            d = lax.dot_general(vals, us[...], nt, preferred_element_type=jnp.float32)
            l_buf[...] += jnp.sum(p, axis=0, keepdims=True)
            e_buf[...] += jnp.sum(p * d, axis=0, keepdims=True)
            s_buf[at, :] = p
            d_buf[at, :] = d

        @pl.loop(0, prompt_blocks, unroll=True)
        def _(j):
            weights(kp[1, k, key_rows(j), :], key_rows(j))

        ticks(3)

        @pl.loop(0, resp_blocks, unroll=True)
        def _(j):
            weights(kr[1, k, b, key_rows(j), :], key_rows(prompt_blocks + j))

        ticks(4)
        inverse = 1.0 / l_buf[...]
        delta = e_buf[...] * inverse

        def grads(keys, at):
            p = s_buf[at, :] * inverse
            ds = (p * (d_buf[at, :] - delta)).astype(jnp.bfloat16)
            dv = jnp.dot(p.astype(jnp.bfloat16), us[...], preferred_element_type=jnp.float32)
            dk = jnp.dot(ds, qs[...], preferred_element_type=jnp.float32) * SCALE
            qt_buf[...] += jnp.dot(keys.T, ds, preferred_element_type=jnp.float32)
            return dk, dv

        @pl.loop(0, prompt_blocks, unroll=True)
        def _(j):
            at = key_rows(j)
            pair = grads(kp[0, k, at, :], at)
            for kind in range(2):
                if b == 0:
                    tp[kind, k, at, :] = pair[kind]
                else:
                    tp[kind, k, at, :] += pair[kind]

        ticks(5)

        @pl.loop(0, resp_blocks, unroll=True)
        def _(j):
            at = key_rows(j)
            pair = grads(kr[0, k, b, at, :], key_rows(prompt_blocks + j))
            for kind in range(2):
                tr[kind, k, b, at, :] = pair[kind]

        ticks(6)
        result = (qt_buf[...].T * SCALE).astype(jnp.bfloat16)
        for source in range(2):
            for g in range(members):
                start = source * half + g * rrows
                dq[source, b, :, pl.ds((k * members + g) * HEAD_DIM, HEAD_DIM)] = result[
                    start : start + rrows
                ]
        cols = pl.ds(k * span, span)
        to = query_columns(side, k)
        remote(
            dq.at[1 - side, b, :, cols], gq.at[b, :, to], gsem.at[0], gsem.at[1], across
        ).start()
        pltpu.make_async_copy(dq.at[side, b, :, cols], gq.at[b, :, to], gsem.at[2]).start()

    def needs(unit):
        k, b = units[unit]
        return [(k, 0), (k, 1)] if b == 0 else [(k, 2)]

    def yields(unit):
        k, b = units[unit]
        return [(k, 1)] if b == 0 else [(k, 0), (k, 2)]

    def ready(unit):
        k, b = units[unit]
        for pair in needs(unit):
            shared(*pair).wait_recv()
        query_crossing(k, b, 1 - side).wait_recv()

    last = len(units) - 1
    for pair in needs(0):
        cross(*pair)
    landed(kp.at[:, :, side_rows(0, side), :], 2)
    landed(kr.at[:, :, :, side_rows(1, side), :], 3)
    for pair in needs(0):
        fan(*pair)
    for pair in needs(1):
        cross(*pair)
    landed(quf, 4)
    query_cross(*units[0])
    for unit in range(2, last + 1):
        for pair in needs(unit):
            cross(*pair)
    for unit in range(1, last + 1):
        query_cross(*units[unit])
    arrive(0, 0)
    fan(0, 2)
    arrive(0, 1)
    for pair in needs(2):
        fan(*pair)
    landed(quh.at[:, side], 5)
    ready(0)
    for unit in range(last + 1):
        k, b = units[unit]

        def ticks(at, unit=unit, k=k, b=b):
            if at == 2 and unit + 3 <= last:
                for pair in needs(unit + 3):
                    fan(*pair)
            if at == 4 and unit < last:
                for pair in needs(unit + 1):
                    arrive(*pair)
            if at == 2 and unit > 0:
                for pair in yields(unit - 1):
                    push(*pair)
            if at == 5 and b == 1:
                meet(k, 0)
            if at == 6:
                meet(k, b + 1)
                if unit == last:
                    push(k, 0)

        compute(unit, ticks)
        if unit < last:
            ready(unit + 1)
    for pair in yields(last):
        if pair[1] > 0:
            push(*pair)
    for unit in range(last + 1):
        for pair in yields(unit):
            finish(*pair)
    drain()
    close()


def key_block(prompt, resp):
    size = 256
    while prompt % size or resp % size:
        size //= 2
    return size


def chunks_of(array):
    return 4 if array.size > 1 << 18 else 1


def settle_kernel(*refs):
    count = (len(refs) - 2) // 4
    sources, targets = refs[:count], refs[count : 2 * count]
    holds, wides = refs[2 * count : 3 * count], refs[3 * count : 4 * count]
    taken, given = refs[4 * count :]
    pieces = []
    for source, target, hold, wide in zip(sources, targets, holds, wides):
        chunks = chunks_of(source)
        step = source.shape[-1] // chunks
        for c in range(chunks):
            cut = (slice(None),) * (len(source.shape) - 1) + (pl.ds(c * step, step),)
            i = len(pieces)
            taking = pltpu.make_async_copy(source.at[cut], hold.at[cut], taken.at[i])
            taking.start()
            giving = pltpu.make_async_copy(wide.at[cut], target.at[cut], given.at[i])
            pieces.append((taking, giving, hold, wide, cut))
    for taking, giving, hold, wide, cut in pieces:
        taking.wait()
        wide[cut] = hold[cut].astype(wide.dtype)
        giving.start()
    for piece in pieces:
        piece[1].wait()


def settle(*arrays):
    hbm = pl.BlockSpec(memory_space=pl.ANY)
    dma = pltpu.SemaphoreType.DMA
    pieces = sum(chunks_of(x) for x in arrays)
    return pl.pallas_call(
        settle_kernel,
        out_shape=tuple(jax.ShapeDtypeStruct(x.shape, jnp.float32) for x in arrays),
        in_specs=[hbm] * len(arrays),
        out_specs=(hbm,) * len(arrays),
        scratch_shapes=[pltpu.VMEM(x.shape, x.dtype) for x in arrays]
        + [pltpu.VMEM(x.shape, jnp.float32) for x in arrays]
        + [dma((pieces,)), dma((pieces,))],
        compiler_params=pltpu.CompilerParams(vmem_limit_bytes=60 * MIB),
        name="settle",
    )(*arrays)


def local(prompt_keys, prompt_values, queries, resp_keys, resp_values, cotangent, lengths):
    devices = lax.axis_size("ctx")
    groups = devices // 4
    prows, columns = prompt_keys.shape
    rows, wide = queries.shape[1], queries.shape[2] // 2
    heads = columns // 2 // HEAD_DIM
    prompt, resp = prows * devices, rows * devices
    smem = pl.BlockSpec(memory_space=pltpu.SMEM)
    hbm = pl.BlockSpec(memory_space=pl.ANY)
    shape = jax.ShapeDtypeStruct
    bf16, f32 = jnp.bfloat16, jnp.float32
    vmem, dma = pltpu.VMEM, pltpu.SemaphoreType.DMA
    block = key_block(prompt, resp)
    lanes = 2 * rows * (wide // HEAD_DIM) // heads
    total = prompt + resp
    both, one = len(offsets(groups, (1, -1))), len(offsets(groups, (1,)))
    outs = pl.pallas_call(
        functools.partial(fused_kernel, groups, block),
        out_shape=(
            shape((2, rows, 2 * wide), bf16),
            shape((2, rows, columns), f32), shape((2, rows, columns), f32),
            shape((prows, columns), f32), shape((prows, columns), f32),
        ),
        in_specs=[smem] + [hbm] * 6,
        out_specs=(hbm,) * 5,
        scratch_shapes=[
            vmem((2, heads, prompt, HEAD_DIM), bf16),
            vmem((2, heads, 2, resp, HEAD_DIM), bf16),
            vmem((heads, 2, prows, HEAD_DIM), bf16),
            vmem((heads, 2, 2, rows, HEAD_DIM), bf16),
            vmem((resp, 1), jnp.int32),
            vmem((2, 2, 2, rows, wide), bf16), vmem((2, 2, rows, wide), bf16),
            vmem((lanes, HEAD_DIM), bf16), vmem((lanes, HEAD_DIM), bf16),
            vmem((total, lanes), f32), vmem((total, lanes), f32),
            vmem((HEAD_DIM, lanes), f32),
            vmem((1, lanes), f32), vmem((1, lanes), f32), vmem((1, lanes), f32),
            vmem((2, heads, prompt, HEAD_DIM), f32),
            vmem((2, heads, 2, resp, HEAD_DIM), f32),
            vmem((2, heads, prompt // 2, HEAD_DIM), f32),
            vmem((2, heads, 2, resp // 2, HEAD_DIM), f32),
            vmem((heads, both + 1, 2, 2, prows, HEAD_DIM), bf16),
            vmem((heads, 2, one + 1, 2, 2, rows, HEAD_DIM), bf16),
            vmem((heads, 2, groups, 2, prows, HEAD_DIM), bf16),
            vmem((heads, 2, 2, groups, 2, rows, HEAD_DIM), bf16),
            vmem((heads, 2, 2, prows + 2 * rows, HEAD_DIM), f32),
            vmem((2, 2, rows, wide), bf16),
            dma((6,)), dma((2,)), dma((3, heads)), dma((1,)), dma((heads, 2)),
            dma((heads, both)), dma((heads, one)), dma((3, heads, groups)), dma((3,)),
            dma((2,)), dma((3, heads)), dma((2,)), dma((3, heads)),
            dma((both + 1,)), dma((one + 1,)), dma((3, heads, groups)), dma((1,)), dma((3,)),
        ],
        compiler_params=pltpu.CompilerParams(
            collective_id=0, has_side_effects=True, vmem_limit_bytes=60 * MIB
        ),
        name="fused",
    )(lengths, prompt_keys, prompt_values, resp_keys, resp_values, queries, cotangent)
    return settle(*outs)


def solution(mesh):
    placed = (
        P(("pairs", "ctx"), None),
        P(("pairs", "ctx"), None),
        P("pairs", "ctx", None),
        P("pairs", "ctx", None),
        P("pairs", "ctx", None),
        P("pairs", "ctx", None),
        P("pairs"),
    )
    return jax.shard_map(
        local,
        mesh=mesh,
        in_specs=placed,
        out_specs=(
            P("pairs", "ctx", None),
            P("pairs", "ctx", None),
            P("pairs", "ctx", None),
            P(("pairs", "ctx"), None),
            P(("pairs", "ctx"), None),
        ),
        check_vma=False,
    )
```

```python
import functools

import jax
import jax.numpy as jnp
from jax import lax
from jax.experimental import pallas as pl
from jax.experimental.pallas import tpu as pltpu
from jax.sharding import PartitionSpec as P

HEAD_DIM = 128
SCALE = HEAD_DIM ** (-0.5)
LOG2E = 1.4426950408889634
MIB = 1024 * 1024
FAR = 3


def remote(src, dst, send, recv, device):
    return pltpu.make_async_remote_copy(
        src_ref=src,
        dst_ref=dst,
        send_sem=send,
        recv_sem=recv,
        device_id={"ctx": device},
        device_id_type=pl.DeviceIdType.MESH,
    )


def offsets(groups, signs):
    order = [3, 2, 1] + list(range(4, groups))
    return [sign * far for far in order if far < groups for sign in signs]


def fused_kernel(
    groups, block, lengths, pk, pv, rk, rv, q, u,
    gq, grk, grv, gpk, gpv,
    kp, kr, bp, br, kpos, quh, quf, qs, us, s_buf, d_buf, qt_buf, m_buf, l_buf, e_buf,
    tp, tr, xp, xr, sp, sr, rp, rr, lp, lr, fb, dq,
    local_sem, ysend, yrecv, qsend, qrecv, asend_p, asend_r, arecv, bsend, lrecv, dsend, drecv,
    csend, crecv, zsend_p, zsend_r, zrecv, fsem, gsem,
):
    me = lax.axis_index("ctx")
    core, side, group = me % 2, (me // 2) % 2, me // 4

    def device(where, y, c):
        return where * 4 + y * 2 + c

    partner = device(group, side, 1 - core)
    across = device(group, 1 - side, core)
    onward, back = me + 4, me - 4
    prows, rrows = pk.shape[0], rk.shape[1]
    heads = kp.shape[1]
    wide = q.shape[2] // 2
    span = wide // heads
    members = span // HEAD_DIM
    inputs = ((pk, rk), (pv, rv))
    outputs = ((gpk, grk), (gpv, grv))
    parts = (0, 1, 2)

    def size_of(part):
        return prows if part == 0 else rrows

    def signs_out(part):
        return (1, -1) if part == 0 else (1,)

    def signs_back(part):
        return (-1, 1) if part == 0 else (-1,)

    def at_row(start, size):
        return pl.ds(pl.multiple_of(start, 16), size)

    def block_rows(part, c, where):
        size = 2 * size_of(part)
        return at_row(c * groups * size + where * size, size)

    def side_rows(part, y):
        size = size_of(part)
        return at_row(core * groups * 2 * size + group * 2 * size + y * size, size)

    def half_rows(part, where):
        size = 2 * size_of(part)
        return at_row(where * size, size)

    def core_rows(part, c):
        size = groups * 2 * size_of(part)
        return at_row(c * size, size)

    def pick(pair, k, part):
        return pair[0].at[:, k] if part == 0 else pair[1].at[:, k, part - 1]

    def stack(pair, k, part):
        return pair[0].at[k] if part == 0 else pair[1].at[k, part - 1]

    def head_columns(y, k):
        return pl.ds(pl.multiple_of((y * heads + k) * HEAD_DIM, HEAD_DIM), HEAD_DIM)

    def query_columns(y, k):
        return pl.ds(pl.multiple_of((y * heads + k) * span, span), span)

    def given(kind, part, cols):
        ref = inputs[kind][min(part, 1)]
        return ref.at[:, cols] if part == 0 else ref.at[part - 1, :, cols]

    def valid(where):
        return jnp.logical_and(where >= 0, where < groups)

    units = [(k, b) for k in range(heads) for b in range(2)]
    order = [(k, part) for k in range(heads) for part in parts]

    for c in range(2):
        for where in range(groups):
            @pl.when(where > group)
            def _(c=c, where=where):
                empty = jnp.zeros((2, heads, 2, 2 * rrows, HEAD_DIM), kr.dtype)
                kr[:, :, :, pl.ds((c * groups + where) * 2 * rrows, 2 * rrows), :] = empty
    for ref in (rp, rr, lp, lr):
        ref[...] = jnp.zeros_like(ref)

    barrier = pltpu.get_barrier_semaphore()
    peers = [partner, across] + [
        device((group + i) % groups, y, core) for i in range(1, groups) for y in range(2)
    ]
    for other in peers:
        pl.semaphore_signal(
            barrier, inc=1, device_id={"ctx": other}, device_id_type=pl.DeviceIdType.MESH
        )

    for k, part in order:
        for kind in range(2):
            pltpu.make_async_copy(
                given(kind, part, head_columns(1 - side, k)),
                stack((bp, br), k, part).at[kind], local_sem.at[min(part, 1)],
            ).start()
            pltpu.make_async_copy(
                given(kind, part, head_columns(side, k)),
                pick((kp, kr), k, part).at[kind, side_rows(part, side), :],
                local_sem.at[2 + min(part, 1)],
            ).start()
    wide_own = pl.ds(pl.multiple_of(side * wide, wide), wide)
    wide_far = pl.ds(pl.multiple_of((1 - side) * wide, wide), wide)
    for i, src in enumerate((q, u)):
        pltpu.make_async_copy(src.at[:, :, wide_far], quf.at[i], local_sem.at[4]).start()
        pltpu.make_async_copy(src.at[:, :, wide_own], quh.at[i, side], local_sem.at[5]).start()

    for c in range(2):
        for where in range(groups):
            for y in range(2):
                start = ((c * groups + where) * 2 + y) * rrows
                kpos[pl.ds(start, rrows), :] = device(where, y, c) * rrows + lax.broadcasted_iota(
                    jnp.int32, (rrows, 1), 0
                )

    def landed(ref, i):
        pltpu.make_async_copy(ref, ref, local_sem.at[i]).wait()

    def hello():
        pl.semaphore_wait(barrier, len(peers))

    hello()
    landed(bp, 0)
    landed(br, 1)

    def cross(k, part, kind, y=side):
        src = stack((bp, br), k, part).at[kind]
        dst = pick((kp, kr), k, part).at[kind, side_rows(part, y), :]
        return remote(src, dst, ysend.at[min(part, 1)], yrecv.at[kind, part, k], across)

    def query_crossing(k, b, y):
        ref = quh.at[:, y, b, :, pl.ds(k * span, span)]
        return remote(ref, ref, qsend.at[0], qrecv.at[k, b], across)

    def query_cross(k, b):
        cols = pl.ds(k * span, span)
        for i in range(2):
            remote(
                quf.at[i, b, :, cols], quh.at[i, side, b, :, cols],
                qsend.at[0], qrecv.at[k, b], across,
            ).start()

    def shared(k, part, kind):
        ref = pick((kp, kr), k, part).at[kind, core_rows(part, core), :]
        return remote(ref, ref, dsend.at[min(part, 1)], drecv.at[kind, part, k], partner)

    def fanned(part, i):
        return asend_p.at[i] if part == 0 else asend_r.at[i]

    def fan(k, part, kind):
        cross(k, part, kind, 1 - side).wait_recv()
        ref = pick((kp, kr), k, part).at[kind, block_rows(part, core, group), :]
        for i, delta in enumerate(offsets(groups, signs_out(part))):
            if delta == FAR:
                continue
            to = group + delta
            copy = remote(
                ref, ref, fanned(part, i), arecv.at[kind, part, k, group], device(to, side, core)
            )
            pl.when(valid(to))(copy.start)

    def spread(k, part, kind):
        near = pick((kp, kr), k, part).at[kind, side_rows(part, side), :]
        far = stack((bp, br), k, part).at[kind]
        for i, delta in enumerate(offsets(groups, signs_out(part))):
            if delta == FAR:
                continue
            to = group + delta
            sem, got = fanned(part, i), arecv.at[kind, part, k, group]

            @pl.when(valid(to))
            def _(to=to, sem=sem, got=got):
                remote(near, near, sem, got, device(to, side, core)).start()
                remote(far, near, sem, got, device(to, 1 - side, core)).start()

    def came(k, part, kind, origin):
        ref = pick((kp, kr), k, part).at[kind, block_rows(part, core, origin), :]
        return remote(ref, ref, bsend.at[min(part, 1)], arecv.at[kind, part, k, origin], onward)

    def relay(k, part, kind):
        if groups <= FAR:
            return
        origin = group - FAR + 1
        copy = came(k, part, kind, origin)

        @pl.when(jnp.logical_and(origin >= 0, group + 1 < groups))
        def _():
            copy.wait_recv()
            copy.start()

    def arrive(k, part, kind):
        if (k, part) in spread_parts and kind == 0:
            cross(k, part, kind, 1 - side).wait_recv()
        for delta in sorted(offsets(groups, signs_out(part)), key=abs):
            origin = group - delta
            waits = valid(origin)
            if delta == FAR - 1 and groups > FAR:
                waits = jnp.logical_and(waits, group + 1 >= groups)
            pl.when(waits)(came(k, part, kind, origin).wait_recv)
        shared(k, part, kind).start()

    spread_parts = ((0, 0), (0, 1))

    def met(k, part):
        ref = pick((tp, tr), k, part).at[:, core_rows(part, 1 - core), :]
        return remote(
            ref, pick((xp, xr), k, part), csend.at[min(part, 1)], crecv.at[part, k], partner
        )

    def meet(k, part):
        met(k, part).start()

    def total(kind, k, part, where):
        mine = pick((tp, tr), k, part).at[kind, block_rows(part, core, where), :]
        other = pick((xp, xr), k, part).at[kind, half_rows(part, where), :]
        return mine[...] + other[...]

    def returns(part):
        return offsets(groups, signs_back(part)) + [0]

    def returned(part, i):
        return zsend_p.at[i] if part == 0 else zsend_r.at[i]

    def push(k, part, gathers):
        size = size_of(part)
        passing = stack((lp, lr), k, part)
        for i, delta in enumerate(returns(part)):
            to = group + delta
            if (delta == 1 - FAR and groups > FAR) != gathers:
                continue
            out = stack((sp, sr), k, part).at[i]
            if delta == -FAR:
                copies = [remote(out, passing, returned(part, i), lrecv.at[part, k], back)]
            else:
                sides = range(2) if delta else (1 - side,)
                copies = [
                    remote(
                        out.at[y], stack((rp, rr), k, part).at[side, group], returned(part, i),
                        zrecv.at[part, k, group], device(to, y, core),
                    )
                    for y in sides
                ]
            if gathers:
                copy = remote(out, passing, returned(part, i), lrecv.at[part, k], back)
                pl.when(jnp.logical_and(to >= 0, group + 1 < groups))(copy.wait_recv)

            @pl.when(valid(to))
            def _(to=to, out=out, copies=copies):
                for kind in range(2):
                    value = total(kind, k, part, to)
                    for y in range(2):
                        piece = value[y * size : (y + 1) * size]
                        if gathers:
                            piece = piece + passing[y, kind].astype(jnp.float32)
                        out[y, kind] = piece.astype(jnp.bfloat16)
                for copy in copies:
                    copy.start()

    starts = (0, prows, prows + rrows)

    def finish(k, part):
        got = stack((rp, rr), k, part)
        size = size_of(part)
        for delta in returns(part):
            if delta == -FAR:
                continue
            origin = group - delta
            slot = got.at[:, origin] if delta else got.at[0, origin]
            copy = remote(slot, slot, fanned(part, 0), zrecv.at[part, k, origin], partner)
            pl.when(valid(origin))(copy.wait_recv)
        rows = pl.ds(starts[part], size)
        near = at_row(group * 2 * size + side * size, size)
        for kind in range(2):
            mine = pick((tp, tr), k, part).at[kind, side_rows(part, side), :]
            own = mine[...] + pick((xp, xr), k, part).at[kind, near, :][...]
            out = outputs[kind][min(part, 1)]
            for y in range(2):
                value = jnp.where(side == y, own, jnp.zeros_like(own))
                for origin in range(groups):
                    value = value + got[y, origin, kind].astype(jnp.float32)
                fb[k, kind, y, rows, :] = value
                cols = pl.ds((y * heads + k) * HEAD_DIM, HEAD_DIM)
                dst = out.at[:, cols] if part == 0 else out.at[part - 1, :, cols]
                pltpu.make_async_copy(fb.at[k, kind, y, rows, :], dst, fsem.at[0]).start()

    def drain():
        remote(bp, bp, ysend.at[0], ysend.at[0], across).wait_send()
        remote(br, br, ysend.at[1], ysend.at[1], across).wait_send()
        remote(quf, quf, qsend.at[0], qsend.at[0], across).wait_send()
        ref = kp.at[:, :, core_rows(0, core), :]
        remote(ref, ref, dsend.at[0], dsend.at[0], partner).wait_send()
        ref = kr.at[:, :, :, core_rows(1, core), :]
        remote(ref, ref, dsend.at[1], dsend.at[1], partner).wait_send()
        ref = tp.at[:, :, core_rows(0, 1 - core), :]
        remote(ref, ref, csend.at[0], csend.at[0], partner).wait_send()
        ref = tr.at[:, :, :, core_rows(1, 1 - core), :]
        remote(ref, ref, csend.at[1], csend.at[1], partner).wait_send()
        for part in range(2):
            for i, delta in enumerate(offsets(groups, signs_out(part))):
                if part == 0:
                    ref = kp.at[:, :, block_rows(0, core, group), :]
                else:
                    ref = kr.at[:, :, :, block_rows(1, core, group), :]
                sem = fanned(part, i)
                if delta != FAR:
                    pl.when(valid(group + delta))(remote(ref, ref, sem, sem, across).wait_send)
                    continue
                origin = group - FAR + 1
                if part == 0:
                    ref = kp.at[:, :, block_rows(0, core, origin), :]
                else:
                    ref = kr.at[:, :, :, block_rows(1, core, origin), :]
                sem = bsend.at[part]
                pl.when(jnp.logical_and(origin >= 0, group + 1 < groups))(
                    remote(ref, ref, sem, sem, across).wait_send
                )
            for i, delta in enumerate(returns(part)):
                ref = sp.at[:, i] if part == 0 else sr.at[:, :, i]
                if delta == 0:
                    ref = sp.at[:, i, 0] if part == 0 else sr.at[:, :, i, 0]
                sem = returned(part, i)
                pl.when(valid(group + delta))(remote(ref, ref, sem, sem, across).wait_send)

    def close():
        ref = dq.at[0]
        remote(ref, ref, gsem.at[0], gsem.at[1], across).wait()
        pltpu.make_async_copy(ref, ref, gsem.at[2]).wait()
        pltpu.make_async_copy(fb, fb, fsem.at[0]).wait()

    half = members * rrows
    lanes = 2 * half
    prompt_blocks = kp.shape[2] // block
    resp_blocks = kr.shape[3] // block
    factor = SCALE * LOG2E
    lane = lax.broadcasted_iota(jnp.int32, (1, lanes), 1)
    row_of = lax.rem(lane, rrows)
    first_row = device(group, 0, core) * rrows
    positions = first_row + row_of + jnp.where(lane < half, 0, 2 * rrows)
    row_iota = lax.broadcasted_iota(jnp.int32, (rrows, 1), 0)
    nt = (((1,), (1,)), ((), ()))

    def key_rows(j):
        return pl.ds(pl.multiple_of(j * block, block), block)

    def compute(unit, ticks):
        k, b = units[unit]
        length = lengths[b]
        for source in range(2):
            live = first_row + source * 2 * rrows + row_iota < length
            for g in range(members):
                cols = pl.ds((k * members + g) * HEAD_DIM, HEAD_DIM)
                at = pl.ds(source * half + g * rrows, rrows)
                qs[at, :] = quh[0, source, b, :, cols]
                rows = quh[1, source, b, :, cols]
                us[at, :] = jnp.where(live, rows, jnp.zeros_like(rows))
        m_buf[...] = jnp.full_like(m_buf, -jnp.inf)
        l_buf[...] = jnp.zeros_like(l_buf)
        e_buf[...] = jnp.zeros_like(e_buf)
        qt_buf[...] = jnp.zeros_like(qt_buf)
        ticks(0)

        def scores(keys, at, j, causal):
            s = lax.dot_general(keys, qs[...], nt, preferred_element_type=jnp.float32)
            if causal:
                s = jnp.where(kpos[key_rows(j), :] <= positions, s, -jnp.inf)
            s_buf[at, :] = s
            m_buf[...] = jnp.maximum(m_buf[...], jnp.max(s, axis=0, keepdims=True))

        @pl.loop(0, prompt_blocks, unroll=True)
        def _(j):
            scores(kp[0, k, key_rows(j), :], key_rows(j), j, False)

        ticks(1)

        @pl.loop(0, resp_blocks, unroll=True)
        def _(j):
            scores(kr[0, k, b, key_rows(j), :], key_rows(prompt_blocks + j), j, True)

        ticks(2)
        shift = m_buf[...] * factor

        def weights(vals, at):
            p = jnp.exp2(s_buf[at, :] * factor - shift)
            d = lax.dot_general(vals, us[...], nt, preferred_element_type=jnp.float32)
            l_buf[...] += jnp.sum(p, axis=0, keepdims=True)
            e_buf[...] += jnp.sum(p * d, axis=0, keepdims=True)
            s_buf[at, :] = p
            d_buf[at, :] = d

        @pl.loop(0, prompt_blocks, unroll=True)
        def _(j):
            weights(kp[1, k, key_rows(j), :], key_rows(j))

        ticks(3)

        @pl.loop(0, resp_blocks, unroll=True)
        def _(j):
            weights(kr[1, k, b, key_rows(j), :], key_rows(prompt_blocks + j))

        ticks(4)
        inverse = 1.0 / l_buf[...]
        delta = e_buf[...] * inverse

        def grads(keys, at):
            p = s_buf[at, :] * inverse
            ds = (p * (d_buf[at, :] - delta)).astype(jnp.bfloat16)
            dv = jnp.dot(p.astype(jnp.bfloat16), us[...], preferred_element_type=jnp.float32)
            dk = jnp.dot(ds, qs[...], preferred_element_type=jnp.float32) * SCALE
            qt_buf[...] += jnp.dot(keys.T, ds, preferred_element_type=jnp.float32)
            return dk, dv

        @pl.loop(0, prompt_blocks, unroll=True)
        def _(j):
            at = key_rows(j)
            pair = grads(kp[0, k, at, :], at)
            for kind in range(2):
                if b == 0:
                    tp[kind, k, at, :] = pair[kind]
                else:
                    tp[kind, k, at, :] += pair[kind]

        ticks(5)

        @pl.loop(0, resp_blocks, unroll=True)
        def _(j):
            at = key_rows(j)
            pair = grads(kr[0, k, b, at, :], key_rows(prompt_blocks + j))
            for kind in range(2):
                tr[kind, k, b, at, :] = pair[kind]

        ticks(6)
        result = (qt_buf[...].T * SCALE).astype(jnp.bfloat16)
        for source in range(2):
            for g in range(members):
                start = source * half + g * rrows
                dq[source, b, :, pl.ds((k * members + g) * HEAD_DIM, HEAD_DIM)] = result[
                    start : start + rrows
                ]
        cols = pl.ds(k * span, span)
        to = query_columns(side, k)
        remote(
            dq.at[1 - side, b, :, cols], gq.at[b, :, to], gsem.at[0], gsem.at[1], across
        ).start()
        pltpu.make_async_copy(dq.at[side, b, :, cols], gq.at[b, :, to], gsem.at[2]).start()

    def needs(unit):
        k, b = units[unit]
        return [(k, 0), (k, 1)] if b == 0 else [(k, 2)]

    def yields(unit):
        k, b = units[unit]
        return [(k, 1)] if b == 0 else [(k, 0), (k, 2)]

    def ready(unit):
        k, b = units[unit]
        for pair in needs(unit):
            shared(*pair, 0).wait_recv()
        query_crossing(k, b, 1 - side).wait_recv()

    last = len(units) - 1
    landed(kp.at[:, :, side_rows(0, side), :], 2)
    landed(kr.at[:, :, :, side_rows(1, side), :], 3)
    for pair in spread_parts:
        spread(*pair, 0)
        cross(*pair, 0).start()
    for pair in spread_parts:
        cross(*pair, 1).start()
    for pair in needs(1):
        for kind in range(2):
            cross(*pair, kind).start()
    landed(quf, 4)
    query_cross(*units[0])
    for unit in range(2, last + 1):
        for pair in needs(unit):
            for kind in range(2):
                cross(*pair, kind).start()
    for unit in range(1, last + 1):
        query_cross(*units[unit])
    for pair in spread_parts:
        fan(*pair, 1)
    for pair in spread_parts:
        relay(*pair, 0)
    for kind in range(2):
        fan(0, 2, kind)
    for pair in spread_parts:
        arrive(*pair, 0)
    for pair in spread_parts:
        relay(*pair, 1)
    landed(quh.at[:, side], 5)
    ready(0)
    for unit in range(last + 1):
        k, b = units[unit]

        def ticks(at, unit=unit, k=k, b=b):
            if at == 0 and unit < last:
                for kind in range(2):
                    for pair in needs(unit + 1):
                        relay(*pair, kind)
            if unit == 0 and at == 1:
                for pair in needs(2):
                    for kind in range(2):
                        fan(*pair, kind)
                arrive(0, 0, 1)
            if at == 2:
                if unit == 0:
                    arrive(0, 1, 1)
                for pair in needs(unit):
                    shared(*pair, 1).wait_recv()
            if at == 3 and unit + 3 <= last:
                for pair in needs(unit + 3):
                    for kind in range(2):
                        fan(*pair, kind)
            if at in (4, 5) and unit < last:
                for pair in needs(unit + 1):
                    arrive(*pair, at - 4)
            if at == 2 and unit > 0:
                for pair in yields(unit - 1):
                    met(*pair).wait_recv()
                    push(*pair, False)
            if at == 2 and unit > 1:
                for pair in yields(unit - 2):
                    push(*pair, True)
            if at == 5 and b == 1:
                meet(k, 0)
            if at == 6:
                meet(k, b + 1)
                if unit == last:
                    for pair in yields(unit - 1):
                        push(*pair, True)
                    met(k, 0).wait_recv()
                    push(k, 0, False)

        compute(unit, ticks)
        if unit < last:
            ready(unit + 1)
    for pair in yields(last):
        if pair[1] > 0:
            met(*pair).wait_recv()
            push(*pair, False)
    for pair in yields(last):
        push(*pair, True)
    for unit in range(last + 1):
        for pair in yields(unit):
            finish(*pair)
    drain()
    close()


def key_block(prompt, resp):
    size = 256
    while prompt % size or resp % size:
        size //= 2
    return size


def chunks_of(array):
    return 4 if array.size > 1 << 18 else 1


def settle_kernel(*refs):
    count = (len(refs) - 2) // 4
    sources, targets = refs[:count], refs[count : 2 * count]
    holds, wides = refs[2 * count : 3 * count], refs[3 * count : 4 * count]
    taken, given = refs[4 * count :]
    pieces = []
    for source, target, hold, wide in zip(sources, targets, holds, wides):
        chunks = chunks_of(source)
        step = source.shape[-1] // chunks
        for c in range(chunks):
            cut = (slice(None),) * (len(source.shape) - 1) + (pl.ds(c * step, step),)
            i = len(pieces)
            taking = pltpu.make_async_copy(source.at[cut], hold.at[cut], taken.at[i])
            taking.start()
            giving = pltpu.make_async_copy(wide.at[cut], target.at[cut], given.at[i])
            pieces.append((taking, giving, hold, wide, cut))
    for taking, giving, hold, wide, cut in pieces:
        taking.wait()
        wide[cut] = hold[cut].astype(wide.dtype)
        giving.start()
    for piece in pieces:
        piece[1].wait()


def settle(*arrays):
    hbm = pl.BlockSpec(memory_space=pl.ANY)
    dma = pltpu.SemaphoreType.DMA
    pieces = sum(chunks_of(x) for x in arrays)
    return pl.pallas_call(
        settle_kernel,
        out_shape=tuple(jax.ShapeDtypeStruct(x.shape, jnp.float32) for x in arrays),
        in_specs=[hbm] * len(arrays),
        out_specs=(hbm,) * len(arrays),
        scratch_shapes=[pltpu.VMEM(x.shape, x.dtype) for x in arrays]
        + [pltpu.VMEM(x.shape, jnp.float32) for x in arrays]
        + [dma((pieces,)), dma((pieces,))],
        compiler_params=pltpu.CompilerParams(vmem_limit_bytes=60 * MIB),
        name="settle",
    )(*arrays)


def local(prompt_keys, prompt_values, queries, resp_keys, resp_values, cotangent, lengths):
    devices = lax.axis_size("ctx")
    groups = devices // 4
    prows, columns = prompt_keys.shape
    rows, wide = queries.shape[1], queries.shape[2] // 2
    heads = columns // 2 // HEAD_DIM
    prompt, resp = prows * devices, rows * devices
    smem = pl.BlockSpec(memory_space=pltpu.SMEM)
    hbm = pl.BlockSpec(memory_space=pl.ANY)
    shape = jax.ShapeDtypeStruct
    bf16, f32 = jnp.bfloat16, jnp.float32
    vmem, dma = pltpu.VMEM, pltpu.SemaphoreType.DMA
    block = key_block(prompt, resp)
    lanes = 2 * rows * (wide // HEAD_DIM) // heads
    total = prompt + resp
    both, one = len(offsets(groups, (1, -1))), len(offsets(groups, (1,)))
    outs = pl.pallas_call(
        functools.partial(fused_kernel, groups, block),
        out_shape=(
            shape((2, rows, 2 * wide), bf16),
            shape((2, rows, columns), f32), shape((2, rows, columns), f32),
            shape((prows, columns), f32), shape((prows, columns), f32),
        ),
        in_specs=[smem] + [hbm] * 6,
        out_specs=(hbm,) * 5,
        scratch_shapes=[
            vmem((2, heads, prompt, HEAD_DIM), bf16),
            vmem((2, heads, 2, resp, HEAD_DIM), bf16),
            vmem((heads, 2, prows, HEAD_DIM), bf16),
            vmem((heads, 2, 2, rows, HEAD_DIM), bf16),
            vmem((resp, 1), jnp.int32),
            vmem((2, 2, 2, rows, wide), bf16), vmem((2, 2, rows, wide), bf16),
            vmem((lanes, HEAD_DIM), bf16), vmem((lanes, HEAD_DIM), bf16),
            vmem((total, lanes), f32), vmem((total, lanes), f32),
            vmem((HEAD_DIM, lanes), f32),
            vmem((1, lanes), f32), vmem((1, lanes), f32), vmem((1, lanes), f32),
            vmem((2, heads, prompt, HEAD_DIM), f32),
            vmem((2, heads, 2, resp, HEAD_DIM), f32),
            vmem((2, heads, prompt // 2, HEAD_DIM), f32),
            vmem((2, heads, 2, resp // 2, HEAD_DIM), f32),
            vmem((heads, both + 1, 2, 2, prows, HEAD_DIM), bf16),
            vmem((heads, 2, one + 1, 2, 2, rows, HEAD_DIM), bf16),
            vmem((heads, 2, groups, 2, prows, HEAD_DIM), bf16),
            vmem((heads, 2, 2, groups, 2, rows, HEAD_DIM), bf16),
            vmem((heads, 2, 2, prows, HEAD_DIM), bf16),
            vmem((heads, 2, 2, 2, rows, HEAD_DIM), bf16),
            vmem((heads, 2, 2, prows + 2 * rows, HEAD_DIM), f32),
            vmem((2, 2, rows, wide), bf16),
            dma((6,)), dma((2,)), dma((2, 3, heads)), dma((1,)), dma((heads, 2)),
            dma((both,)), dma((one,)), dma((2, 3, heads, groups)), dma((2,)), dma((3, heads)),
            dma((2,)), dma((2, 3, heads)), dma((2,)), dma((3, heads)),
            dma((both + 1,)), dma((one + 1,)), dma((3, heads, groups)), dma((1,)), dma((3,)),
        ],
        compiler_params=pltpu.CompilerParams(
            collective_id=0, has_side_effects=True, vmem_limit_bytes=60 * MIB
        ),
        name="fused",
    )(lengths, prompt_keys, prompt_values, resp_keys, resp_values, queries, cotangent)
    return settle(*outs)


def solution(mesh):
    placed = (
        P(("pairs", "ctx"), None),
        P(("pairs", "ctx"), None),
        P("pairs", "ctx", None),
        P("pairs", "ctx", None),
        P("pairs", "ctx", None),
        P("pairs", "ctx", None),
        P("pairs"),
    )
    return jax.shard_map(
        local,
        mesh=mesh,
        in_specs=placed,
        out_specs=(
            P("pairs", "ctx", None),
            P("pairs", "ctx", None),
            P("pairs", "ctx", None),
            P(("pairs", "ctx"), None),
            P(("pairs", "ctx"), None),
        ),
        check_vma=False,
    )
```

```python
import functools

import jax
import jax.numpy as jnp
from jax import lax
from jax.experimental import pallas as pl
from jax.experimental.pallas import tpu as pltpu
from jax.sharding import PartitionSpec as P

HEAD_DIM = 128
SCALE = HEAD_DIM ** (-0.5)
LOG2E = 1.4426950408889634
MIB = 1024 * 1024
FAR = 3


def remote(src, dst, send, recv, device):
    return pltpu.make_async_remote_copy(
        src_ref=src,
        dst_ref=dst,
        send_sem=send,
        recv_sem=recv,
        device_id={"ctx": device},
        device_id_type=pl.DeviceIdType.MESH,
    )


def offsets(groups, signs):
    order = [3, 2, 1] + list(range(4, groups))
    return [sign * far for far in order if far < groups for sign in signs]


def fused_kernel(
    groups, block, lengths, pk, pv, rk, rv, q, u,
    gq, grk, grv, gpk, gpv,
    kp, kr, bp, br, kpos, quh, quf, qs, us, s_buf, d_buf, qt_buf, m_buf, l_buf, e_buf,
    tp, tr, xp, xr, sp, sr, rp, rr, lp, lr, fb, dq,
    local_sem, ysend, yrecv, qsend, qrecv, asend_p, asend_r, arecv, bsend, lrecv, dsend, drecv,
    csend, crecv, zsend_p, zsend_r, zrecv, fsem, gsem,
):
    me = lax.axis_index("ctx")
    core, side, group = me % 2, (me // 2) % 2, me // 4

    def device(where, y, c):
        return where * 4 + y * 2 + c

    partner = device(group, side, 1 - core)
    across = device(group, 1 - side, core)
    onward, back = me + 4, me - 4
    prows, rrows = pk.shape[0], rk.shape[1]
    heads = kp.shape[1]
    wide = q.shape[2] // 2
    span = wide // heads
    members = span // HEAD_DIM
    inputs = ((pk, rk), (pv, rv))
    outputs = ((gpk, grk), (gpv, grv))
    parts = (0, 1, 2)

    def size_of(part):
        return prows if part == 0 else rrows

    def signs_out(part):
        return (1, -1) if part == 0 else (1,)

    def signs_back(part):
        return (-1, 1) if part == 0 else (-1,)

    def at_row(start, size):
        return pl.ds(pl.multiple_of(start, 16), size)

    def block_rows(part, c, where):
        size = 2 * size_of(part)
        return at_row(c * groups * size + where * size, size)

    def side_rows(part, y):
        size = size_of(part)
        return at_row(core * groups * 2 * size + group * 2 * size + y * size, size)

    def half_rows(part, where):
        size = 2 * size_of(part)
        return at_row(where * size, size)

    def core_rows(part, c):
        size = groups * 2 * size_of(part)
        return at_row(c * size, size)

    def pick(pair, k, part):
        return pair[0].at[:, k] if part == 0 else pair[1].at[:, k, part - 1]

    def stack(pair, k, part):
        return pair[0].at[k] if part == 0 else pair[1].at[k, part - 1]

    def head_columns(y, k):
        return pl.ds(pl.multiple_of((y * heads + k) * HEAD_DIM, HEAD_DIM), HEAD_DIM)

    def query_columns(y, k):
        return pl.ds(pl.multiple_of((y * heads + k) * span, span), span)

    def given(kind, part, cols):
        ref = inputs[kind][min(part, 1)]
        return ref.at[:, cols] if part == 0 else ref.at[part - 1, :, cols]

    def valid(where):
        return jnp.logical_and(where >= 0, where < groups)

    units = [(k, b) for k in range(heads) for b in range(2)]
    order = [(k, part) for k in range(heads) for part in parts]

    for c in range(2):
        for where in range(groups):
            @pl.when(where > group)
            def _(c=c, where=where):
                empty = jnp.zeros((2, heads, 2, 2 * rrows, HEAD_DIM), kr.dtype)
                kr[:, :, :, pl.ds((c * groups + where) * 2 * rrows, 2 * rrows), :] = empty
    for ref in (rp, rr, lp, lr):
        ref[...] = jnp.zeros_like(ref)

    barrier = pltpu.get_barrier_semaphore()
    peers = [partner, across] + [
        device((group + i) % groups, y, core) for i in range(1, groups) for y in range(2)
    ]
    for other in peers:
        pl.semaphore_signal(
            barrier, inc=1, device_id={"ctx": other}, device_id_type=pl.DeviceIdType.MESH
        )

    for k, part in order:
        for kind in range(2):
            pltpu.make_async_copy(
                given(kind, part, head_columns(1 - side, k)),
                stack((bp, br), k, part).at[kind], local_sem.at[min(part, 1)],
            ).start()
            pltpu.make_async_copy(
                given(kind, part, head_columns(side, k)),
                pick((kp, kr), k, part).at[kind, side_rows(part, side), :],
                local_sem.at[2 + min(part, 1)],
            ).start()
    wide_own = pl.ds(pl.multiple_of(side * wide, wide), wide)
    wide_far = pl.ds(pl.multiple_of((1 - side) * wide, wide), wide)
    for i, src in enumerate((q, u)):
        pltpu.make_async_copy(src.at[:, :, wide_far], quf.at[i], local_sem.at[4]).start()
        pltpu.make_async_copy(src.at[:, :, wide_own], quh.at[i, side], local_sem.at[5]).start()

    for c in range(2):
        for where in range(groups):
            for y in range(2):
                start = ((c * groups + where) * 2 + y) * rrows
                kpos[pl.ds(start, rrows), :] = device(where, y, c) * rrows + lax.broadcasted_iota(
                    jnp.int32, (rrows, 1), 0
                )

    def landed(ref, i):
        pltpu.make_async_copy(ref, ref, local_sem.at[i]).wait()

    def hello():
        pl.semaphore_wait(barrier, len(peers))

    hello()
    landed(bp, 0)
    landed(br, 1)

    def cross(k, part, kind, y=side):
        src = stack((bp, br), k, part).at[kind]
        dst = pick((kp, kr), k, part).at[kind, side_rows(part, y), :]
        return remote(src, dst, ysend.at[min(part, 1)], yrecv.at[kind, part, k], across)

    def query_cross(i, k, b, y=side):
        cols = pl.ds(k * span, span)
        return remote(
            quf.at[i, b, :, cols], quh.at[i, y, b, :, cols],
            qsend.at[0], qrecv.at[i, k, b], across,
        )

    def shared(k, part, kind):
        ref = pick((kp, kr), k, part).at[kind, core_rows(part, core), :]
        return remote(ref, ref, dsend.at[min(part, 1)], drecv.at[kind, part, k], partner)

    def fanned(part, i):
        return asend_p.at[i] if part == 0 else asend_r.at[i]

    def fan(k, part, kind):
        cross(k, part, kind, 1 - side).wait_recv()
        ref = pick((kp, kr), k, part).at[kind, block_rows(part, core, group), :]
        for i, delta in enumerate(offsets(groups, signs_out(part))):
            if delta == FAR:
                continue
            to = group + delta
            copy = remote(
                ref, ref, fanned(part, i), arecv.at[kind, part, k, group], device(to, side, core)
            )
            pl.when(valid(to))(copy.start)

    def spread(k, part, kind):
        near = pick((kp, kr), k, part).at[kind, side_rows(part, side), :]
        far = stack((bp, br), k, part).at[kind]
        for i, delta in enumerate(offsets(groups, signs_out(part))):
            if delta == FAR:
                continue
            to = group + delta
            sem, got = fanned(part, i), arecv.at[kind, part, k, group]

            @pl.when(valid(to))
            def _(to=to, sem=sem, got=got):
                remote(near, near, sem, got, device(to, side, core)).start()
                remote(far, near, sem, got, device(to, 1 - side, core)).start()

    def came(k, part, kind, origin):
        ref = pick((kp, kr), k, part).at[kind, block_rows(part, core, origin), :]
        return remote(ref, ref, bsend.at[min(part, 1)], arecv.at[kind, part, k, origin], onward)

    def relay(k, part, kind):
        if groups <= FAR:
            return
        origin = group - FAR + 1
        copy = came(k, part, kind, origin)

        @pl.when(jnp.logical_and(origin >= 0, group + 1 < groups))
        def _():
            copy.wait_recv()
            copy.start()

    def arrive(k, part, kind):
        if (k, part) in spread_parts and kind == 0:
            cross(k, part, kind, 1 - side).wait_recv()
        for delta in sorted(offsets(groups, signs_out(part)), key=abs):
            origin = group - delta
            waits = valid(origin)
            if delta == FAR - 1 and groups > FAR:
                waits = jnp.logical_and(waits, group + 1 >= groups)
            pl.when(waits)(came(k, part, kind, origin).wait_recv)
        shared(k, part, kind).start()

    spread_parts = ((0, 0), (0, 1))

    def met(k, part):
        ref = pick((tp, tr), k, part).at[:, core_rows(part, 1 - core), :]
        return remote(
            ref, pick((xp, xr), k, part), csend.at[min(part, 1)], crecv.at[part, k], partner
        )

    def meet(k, part):
        met(k, part).start()

    def total(kind, k, part, where):
        mine = pick((tp, tr), k, part).at[kind, block_rows(part, core, where), :]
        other = pick((xp, xr), k, part).at[kind, half_rows(part, where), :]
        return mine[...] + other[...]

    def returns(part):
        return offsets(groups, signs_back(part)) + [0]

    def returned(part, i):
        return zsend_p.at[i] if part == 0 else zsend_r.at[i]

    def push(k, part, gathers):
        size = size_of(part)
        passing = stack((lp, lr), k, part)
        more = group + 1 < groups
        for i, delta in enumerate(returns(part)):
            to = group + delta
            cond = valid(to)
            if delta == 1 - FAR and groups > FAR:
                cond = jnp.logical_and(cond, more if gathers else jnp.logical_not(more))
            elif gathers:
                continue
            out = stack((sp, sr), k, part).at[i]
            if delta == -FAR:
                copies = [remote(out, passing, returned(part, i), lrecv.at[part, k], back)]
            else:
                sides = range(2) if delta else (1 - side,)
                copies = [
                    remote(
                        out.at[y], stack((rp, rr), k, part).at[side, group], returned(part, i),
                        zrecv.at[part, k, group], device(to, y, core),
                    )
                    for y in sides
                ]
            wait = remote(out, passing, returned(part, i), lrecv.at[part, k], back)

            @pl.when(cond)
            def _(to=to, out=out, copies=copies, wait=wait):
                if gathers:
                    wait.wait_recv()
                for kind in range(2):
                    value = total(kind, k, part, to)
                    for y in range(2):
                        piece = value[y * size : (y + 1) * size]
                        if gathers:
                            piece = piece + passing[y, kind].astype(jnp.float32)
                        out[y, kind] = piece.astype(jnp.bfloat16)
                for copy in copies:
                    copy.start()

    starts = (0, prows, prows + rrows)

    def finish(k, part):
        got = stack((rp, rr), k, part)
        size = size_of(part)
        for delta in returns(part):
            if delta == -FAR:
                continue
            origin = group - delta
            slot = got.at[:, origin] if delta else got.at[0, origin]
            copy = remote(slot, slot, fanned(part, 0), zrecv.at[part, k, origin], partner)
            pl.when(valid(origin))(copy.wait_recv)
        rows = pl.ds(starts[part], size)
        near = at_row(group * 2 * size + side * size, size)
        for kind in range(2):
            mine = pick((tp, tr), k, part).at[kind, side_rows(part, side), :]
            own = mine[...] + pick((xp, xr), k, part).at[kind, near, :][...]
            out = outputs[kind][min(part, 1)]
            for y in range(2):
                value = jnp.where(side == y, own, jnp.zeros_like(own))
                for origin in range(groups):
                    value = value + got[y, origin, kind].astype(jnp.float32)
                fb[k, kind, y, rows, :] = value
                cols = pl.ds((y * heads + k) * HEAD_DIM, HEAD_DIM)
                dst = out.at[:, cols] if part == 0 else out.at[part - 1, :, cols]
                pltpu.make_async_copy(fb.at[k, kind, y, rows, :], dst, fsem.at[0]).start()

    def drain():
        remote(bp, bp, ysend.at[0], ysend.at[0], across).wait_send()
        remote(br, br, ysend.at[1], ysend.at[1], across).wait_send()
        remote(quf, quf, qsend.at[0], qsend.at[0], across).wait_send()
        ref = kp.at[:, :, core_rows(0, core), :]
        remote(ref, ref, dsend.at[0], dsend.at[0], partner).wait_send()
        ref = kr.at[:, :, :, core_rows(1, core), :]
        remote(ref, ref, dsend.at[1], dsend.at[1], partner).wait_send()
        ref = tp.at[:, :, core_rows(0, 1 - core), :]
        remote(ref, ref, csend.at[0], csend.at[0], partner).wait_send()
        ref = tr.at[:, :, :, core_rows(1, 1 - core), :]
        remote(ref, ref, csend.at[1], csend.at[1], partner).wait_send()
        for part in range(2):
            for i, delta in enumerate(offsets(groups, signs_out(part))):
                if part == 0:
                    ref = kp.at[:, :, block_rows(0, core, group), :]
                else:
                    ref = kr.at[:, :, :, block_rows(1, core, group), :]
                sem = fanned(part, i)
                if delta != FAR:
                    pl.when(valid(group + delta))(remote(ref, ref, sem, sem, across).wait_send)
                    continue
                origin = group - FAR + 1
                if part == 0:
                    ref = kp.at[:, :, block_rows(0, core, origin), :]
                else:
                    ref = kr.at[:, :, :, block_rows(1, core, origin), :]
                sem = bsend.at[part]
                pl.when(jnp.logical_and(origin >= 0, group + 1 < groups))(
                    remote(ref, ref, sem, sem, across).wait_send
                )
            for i, delta in enumerate(returns(part)):
                ref = sp.at[:, i] if part == 0 else sr.at[:, :, i]
                if delta == 0:
                    ref = sp.at[:, i, 0] if part == 0 else sr.at[:, :, i, 0]
                sem = returned(part, i)
                pl.when(valid(group + delta))(remote(ref, ref, sem, sem, across).wait_send)

    def close():
        ref = dq.at[0]
        remote(ref, ref, gsem.at[0], gsem.at[1], across).wait()
        pltpu.make_async_copy(ref, ref, gsem.at[2]).wait()
        pltpu.make_async_copy(fb, fb, fsem.at[0]).wait()

    half = members * rrows
    lanes = 2 * half
    prompt_blocks = kp.shape[2] // block
    resp_blocks = kr.shape[3] // block
    factor = SCALE * LOG2E
    lane = lax.broadcasted_iota(jnp.int32, (1, lanes), 1)
    row_of = lax.rem(lane, rrows)
    first_row = device(group, 0, core) * rrows
    positions = first_row + row_of + jnp.where(lane < half, 0, 2 * rrows)
    row_iota = lax.broadcasted_iota(jnp.int32, (rrows, 1), 0)
    nt = (((1,), (1,)), ((), ()))

    def key_rows(j):
        return pl.ds(pl.multiple_of(j * block, block), block)

    def compute(unit, ticks):
        k, b = units[unit]
        length = lengths[b]
        for source in range(2):
            for g in range(members):
                cols = pl.ds((k * members + g) * HEAD_DIM, HEAD_DIM)
                at = pl.ds(source * half + g * rrows, rrows)
                qs[at, :] = quh[0, source, b, :, cols]
        m_buf[...] = jnp.full_like(m_buf, -jnp.inf)
        l_buf[...] = jnp.zeros_like(l_buf)
        e_buf[...] = jnp.zeros_like(e_buf)
        qt_buf[...] = jnp.zeros_like(qt_buf)
        ticks(0)

        def scores(keys, at, j, causal):
            s = lax.dot_general(keys, qs[...], nt, preferred_element_type=jnp.float32)
            if causal:
                s = jnp.where(kpos[key_rows(j), :] <= positions, s, -jnp.inf)
            s_buf[at, :] = s
            m_buf[...] = jnp.maximum(m_buf[...], jnp.max(s, axis=0, keepdims=True))

        @pl.loop(0, prompt_blocks, unroll=True)
        def _(j):
            scores(kp[0, k, key_rows(j), :], key_rows(j), j, False)

        ticks(1)

        @pl.loop(0, resp_blocks, unroll=True)
        def _(j):
            scores(kr[0, k, b, key_rows(j), :], key_rows(prompt_blocks + j), j, True)

        ticks(2)
        for source in range(2):
            live = first_row + source * 2 * rrows + row_iota < length
            for g in range(members):
                cols = pl.ds((k * members + g) * HEAD_DIM, HEAD_DIM)
                at = pl.ds(source * half + g * rrows, rrows)
                rows = quh[1, source, b, :, cols]
                us[at, :] = jnp.where(live, rows, jnp.zeros_like(rows))
        shift = m_buf[...] * factor

        def weights(vals, at):
            p = jnp.exp2(s_buf[at, :] * factor - shift)
            d = lax.dot_general(vals, us[...], nt, preferred_element_type=jnp.float32)
            l_buf[...] += jnp.sum(p, axis=0, keepdims=True)
            e_buf[...] += jnp.sum(p * d, axis=0, keepdims=True)
            s_buf[at, :] = p
            d_buf[at, :] = d

        @pl.loop(0, prompt_blocks, unroll=True)
        def _(j):
            weights(kp[1, k, key_rows(j), :], key_rows(j))

        ticks(3)

        @pl.loop(0, resp_blocks, unroll=True)
        def _(j):
            weights(kr[1, k, b, key_rows(j), :], key_rows(prompt_blocks + j))

        ticks(4)
        inverse = 1.0 / l_buf[...]
        delta = e_buf[...] * inverse

        def grads(keys, at):
            p = s_buf[at, :] * inverse
            ds = (p * (d_buf[at, :] - delta)).astype(jnp.bfloat16)
            dv = jnp.dot(p.astype(jnp.bfloat16), us[...], preferred_element_type=jnp.float32)
            dk = jnp.dot(ds, qs[...], preferred_element_type=jnp.float32) * SCALE
            qt_buf[...] += jnp.dot(keys.T, ds, preferred_element_type=jnp.float32)
            return dk, dv

        @pl.loop(0, prompt_blocks, unroll=True)
        def _(j):
            at = key_rows(j)
            pair = grads(kp[0, k, at, :], at)
            for kind in range(2):
                if b == 0:
                    tp[kind, k, at, :] = pair[kind]
                else:
                    tp[kind, k, at, :] += pair[kind]

        ticks(5)

        @pl.loop(0, resp_blocks, unroll=True)
        def _(j):
            at = key_rows(j)
            pair = grads(kr[0, k, b, at, :], key_rows(prompt_blocks + j))
            for kind in range(2):
                tr[kind, k, b, at, :] = pair[kind]

        ticks(6)
        result = (qt_buf[...].T * SCALE).astype(jnp.bfloat16)
        for source in range(2):
            for g in range(members):
                start = source * half + g * rrows
                dq[source, b, :, pl.ds((k * members + g) * HEAD_DIM, HEAD_DIM)] = result[
                    start : start + rrows
                ]
        cols = pl.ds(k * span, span)
        to = query_columns(side, k)
        remote(
            dq.at[1 - side, b, :, cols], gq.at[b, :, to], gsem.at[0], gsem.at[1], across
        ).start()
        pltpu.make_async_copy(dq.at[side, b, :, cols], gq.at[b, :, to], gsem.at[2]).start()

    def needs(unit):
        k, b = units[unit]
        return [(k, 0), (k, 1)] if b == 0 else [(k, 2)]

    def yields(unit):
        k, b = units[unit]
        return [(k, 1)] if b == 0 else [(k, 0), (k, 2)]

    def ready(unit):
        k, b = units[unit]
        for pair in needs(unit):
            shared(*pair, 0).wait_recv()
        query_cross(0, k, b, 1 - side).wait_recv()

    last = len(units) - 1
    landed(kp.at[:, :, side_rows(0, side), :], 2)
    landed(kr.at[:, :, :, side_rows(1, side), :], 3)
    for pair in spread_parts:
        spread(*pair, 0)
        cross(*pair, 0).start()
    for pair in spread_parts:
        cross(*pair, 1).start()
    for kind in range(2):
        cross(0, 2, kind).start()
    landed(quf, 4)
    query_cross(0, *units[0]).start()
    for kind in range(2):
        for pair in needs(2):
            cross(*pair, kind).start()
    query_cross(1, *units[0]).start()
    for unit in range(3, last + 1):
        for kind in range(2):
            for pair in needs(unit):
                cross(*pair, kind).start()
    for i in range(2):
        query_cross(i, *units[1]).start()
    for unit in range(2, last + 1):
        for i in range(2):
            query_cross(i, *units[unit]).start()
    for pair in spread_parts:
        fan(*pair, 1)
    for pair in spread_parts:
        relay(*pair, 0)
    for kind in range(2):
        fan(0, 2, kind)
    for pair in spread_parts:
        arrive(*pair, 0)
    for pair in spread_parts:
        relay(*pair, 1)
    for kind in range(2):
        for pair in needs(2):
            fan(*pair, kind)
    landed(quh.at[:, side], 5)
    ready(0)
    for unit in range(last + 1):
        k, b = units[unit]

        def ticks(at, unit=unit, k=k, b=b):
            if at == 0 and unit == 0:
                for kind in range(2):
                    relay(0, 2, kind)
            if unit == 0 and at == 1:
                arrive(0, 0, 1)
            if at == 2:
                if unit == 0:
                    arrive(0, 1, 1)
                for pair in needs(unit):
                    shared(*pair, 1).wait_recv()
                query_cross(1, k, b, 1 - side).wait_recv()
            if at == 3 and unit + 3 <= last:
                for pair in needs(unit + 3):
                    for kind in range(2):
                        fan(*pair, kind)
            if at in (4, 5) and unit < last:
                for pair in needs(unit + 1):
                    arrive(*pair, at - 4)
            if at == 2 and unit > 0:
                for pair in yields(unit - 1):
                    met(*pair).wait_recv()
                    push(*pair, False)
            if at == 2 and unit > 1:
                for pair in yields(unit - 2):
                    push(*pair, True)
            if at == 5 and b == 1:
                meet(k, 0)
            if at == 6:
                meet(k, b + 1)
                if unit + 2 <= last:
                    for kind in range(2):
                        for pair in needs(unit + 2):
                            relay(*pair, kind)
                if unit == last:
                    for pair in yields(unit - 1):
                        push(*pair, True)
                    met(k, 0).wait_recv()
                    push(k, 0, False)

        compute(unit, ticks)
        if unit < last:
            ready(unit + 1)
    for pair in yields(last):
        if pair[1] > 0:
            met(*pair).wait_recv()
            push(*pair, False)
    for pair in yields(last):
        push(*pair, True)
    for unit in range(last + 1):
        for pair in yields(unit):
            finish(*pair)
    drain()
    close()


def key_block(prompt, resp):
    size = 256
    while prompt % size or resp % size:
        size //= 2
    return size


def chunks_of(array):
    return 4 if array.size > 1 << 18 else 1


def settle_kernel(*refs):
    count = (len(refs) - 2) // 4
    sources, targets = refs[:count], refs[count : 2 * count]
    holds, wides = refs[2 * count : 3 * count], refs[3 * count : 4 * count]
    taken, given = refs[4 * count :]
    pieces = []
    for source, target, hold, wide in zip(sources, targets, holds, wides):
        chunks = chunks_of(source)
        step = source.shape[-1] // chunks
        for c in range(chunks):
            cut = (slice(None),) * (len(source.shape) - 1) + (pl.ds(c * step, step),)
            i = len(pieces)
            taking = pltpu.make_async_copy(source.at[cut], hold.at[cut], taken.at[i])
            taking.start()
            giving = pltpu.make_async_copy(wide.at[cut], target.at[cut], given.at[i])
            pieces.append((taking, giving, hold, wide, cut))
    for taking, giving, hold, wide, cut in pieces:
        taking.wait()
        wide[cut] = hold[cut].astype(wide.dtype)
        giving.start()
    for piece in pieces:
        piece[1].wait()


def settle(*arrays):
    hbm = pl.BlockSpec(memory_space=pl.ANY)
    dma = pltpu.SemaphoreType.DMA
    pieces = sum(chunks_of(x) for x in arrays)
    return pl.pallas_call(
        settle_kernel,
        out_shape=tuple(jax.ShapeDtypeStruct(x.shape, jnp.float32) for x in arrays),
        in_specs=[hbm] * len(arrays),
        out_specs=(hbm,) * len(arrays),
        scratch_shapes=[pltpu.VMEM(x.shape, x.dtype) for x in arrays]
        + [pltpu.VMEM(x.shape, jnp.float32) for x in arrays]
        + [dma((pieces,)), dma((pieces,))],
        compiler_params=pltpu.CompilerParams(vmem_limit_bytes=60 * MIB),
        name="settle",
    )(*arrays)


def local(prompt_keys, prompt_values, queries, resp_keys, resp_values, cotangent, lengths):
    devices = lax.axis_size("ctx")
    groups = devices // 4
    prows, columns = prompt_keys.shape
    rows, wide = queries.shape[1], queries.shape[2] // 2
    heads = columns // 2 // HEAD_DIM
    prompt, resp = prows * devices, rows * devices
    smem = pl.BlockSpec(memory_space=pltpu.SMEM)
    hbm = pl.BlockSpec(memory_space=pl.ANY)
    shape = jax.ShapeDtypeStruct
    bf16, f32 = jnp.bfloat16, jnp.float32
    vmem, dma = pltpu.VMEM, pltpu.SemaphoreType.DMA
    block = key_block(prompt, resp)
    lanes = 2 * rows * (wide // HEAD_DIM) // heads
    total = prompt + resp
    both, one = len(offsets(groups, (1, -1))), len(offsets(groups, (1,)))
    outs = pl.pallas_call(
        functools.partial(fused_kernel, groups, block),
        out_shape=(
            shape((2, rows, 2 * wide), bf16),
            shape((2, rows, columns), f32), shape((2, rows, columns), f32),
            shape((prows, columns), f32), shape((prows, columns), f32),
        ),
        in_specs=[smem] + [hbm] * 6,
        out_specs=(hbm,) * 5,
        scratch_shapes=[
            vmem((2, heads, prompt, HEAD_DIM), bf16),
            vmem((2, heads, 2, resp, HEAD_DIM), bf16),
            vmem((heads, 2, prows, HEAD_DIM), bf16),
            vmem((heads, 2, 2, rows, HEAD_DIM), bf16),
            vmem((resp, 1), jnp.int32),
            vmem((2, 2, 2, rows, wide), bf16), vmem((2, 2, rows, wide), bf16),
            vmem((lanes, HEAD_DIM), bf16), vmem((lanes, HEAD_DIM), bf16),
            vmem((total, lanes), f32), vmem((total, lanes), f32),
            vmem((HEAD_DIM, lanes), f32),
            vmem((1, lanes), f32), vmem((1, lanes), f32), vmem((1, lanes), f32),
            vmem((2, heads, prompt, HEAD_DIM), f32),
            vmem((2, heads, 2, resp, HEAD_DIM), f32),
            vmem((2, heads, prompt // 2, HEAD_DIM), f32),
            vmem((2, heads, 2, resp // 2, HEAD_DIM), f32),
            vmem((heads, both + 1, 2, 2, prows, HEAD_DIM), bf16),
            vmem((heads, 2, one + 1, 2, 2, rows, HEAD_DIM), bf16),
            vmem((heads, 2, groups, 2, prows, HEAD_DIM), bf16),
            vmem((heads, 2, 2, groups, 2, rows, HEAD_DIM), bf16),
            vmem((heads, 2, 2, prows, HEAD_DIM), bf16),
            vmem((heads, 2, 2, 2, rows, HEAD_DIM), bf16),
            vmem((heads, 2, 2, prows + 2 * rows, HEAD_DIM), f32),
            vmem((2, 2, rows, wide), bf16),
            dma((6,)), dma((2,)), dma((2, 3, heads)), dma((1,)), dma((2, heads, 2)),
            dma((both,)), dma((one,)), dma((2, 3, heads, groups)), dma((2,)), dma((3, heads)),
            dma((2,)), dma((2, 3, heads)), dma((2,)), dma((3, heads)),
            dma((both + 1,)), dma((one + 1,)), dma((3, heads, groups)), dma((1,)), dma((3,)),
        ],
        compiler_params=pltpu.CompilerParams(
            collective_id=0, has_side_effects=True, vmem_limit_bytes=60 * MIB
        ),
        name="fused",
    )(lengths, prompt_keys, prompt_values, resp_keys, resp_values, queries, cotangent)
    return settle(*outs)


def solution(mesh):
    placed = (
        P(("pairs", "ctx"), None),
        P(("pairs", "ctx"), None),
        P("pairs", "ctx", None),
        P("pairs", "ctx", None),
        P("pairs", "ctx", None),
        P("pairs", "ctx", None),
        P("pairs"),
    )
    return jax.shard_map(
        local,
        mesh=mesh,
        in_specs=placed,
        out_specs=(
            P("pairs", "ctx", None),
            P("pairs", "ctx", None),
            P("pairs", "ctx", None),
            P(("pairs", "ctx"), None),
            P(("pairs", "ctx"), None),
        ),
        check_vma=False,
    )
```

```python
import functools

import jax
import jax.numpy as jnp
from jax import lax
from jax.experimental import pallas as pl
from jax.experimental.pallas import tpu as pltpu
from jax.sharding import PartitionSpec as P

HEAD_DIM = 128
SCALE = HEAD_DIM ** (-0.5)
LOG2E = 1.4426950408889634
MIB = 1024 * 1024
FAR = 3


def remote(src, dst, send, recv, device):
    return pltpu.make_async_remote_copy(
        src_ref=src,
        dst_ref=dst,
        send_sem=send,
        recv_sem=recv,
        device_id={"ctx": device},
        device_id_type=pl.DeviceIdType.MESH,
    )


def offsets(groups, signs):
    order = [3, 2, 1] + list(range(4, groups))
    return [sign * far for far in order if far < groups for sign in signs]


def fused_kernel(
    groups, block, lengths, pk, pv, rk, rv, q, u,
    gq, grk, grv, gpk, gpv,
    kp, kr, bp, br, kpos, quh, quf, qs, us, s_buf, d_buf, qt_buf, m_buf, l_buf, e_buf,
    tp, tr, xp, xr, sp, sr, rp, rr, lp, lr, fb, dq,
    local_sem, ysend, yrecv, qsend, qrecv, asend_p, asend_r, arecv, bsend, lrecv, dsend, drecv,
    csend, crecv, zsend_p, zsend_r, zrecv, fsem, gsem,
):
    me = lax.axis_index("ctx")
    core, side, group = me % 2, (me // 2) % 2, me // 4

    def device(where, y, c):
        return where * 4 + y * 2 + c

    partner = device(group, side, 1 - core)
    across = device(group, 1 - side, core)
    onward, back = me + 4, me - 4
    prows, rrows = pk.shape[0], rk.shape[1]
    heads = kp.shape[1]
    wide = q.shape[2] // 2
    span = wide // heads
    members = span // HEAD_DIM
    inputs = ((pk, rk), (pv, rv))
    outputs = ((gpk, grk), (gpv, grv))
    parts = (0, 1, 2)

    def size_of(part):
        return prows if part == 0 else rrows

    def signs_out(part):
        return (1, -1) if part == 0 else (1,)

    def signs_back(part):
        return (-1, 1) if part == 0 else (-1,)

    def at_row(start, size):
        return pl.ds(pl.multiple_of(start, 16), size)

    def block_rows(part, c, where):
        size = 2 * size_of(part)
        return at_row(c * groups * size + where * size, size)

    def side_rows(part, y):
        size = size_of(part)
        return at_row(core * groups * 2 * size + group * 2 * size + y * size, size)

    def half_rows(part, where):
        size = 2 * size_of(part)
        return at_row(where * size, size)

    def core_rows(part, c):
        size = groups * 2 * size_of(part)
        return at_row(c * size, size)

    def pick(pair, k, part):
        return pair[0].at[:, k] if part == 0 else pair[1].at[:, k, part - 1]

    def stack(pair, k, part):
        return pair[0].at[k] if part == 0 else pair[1].at[k, part - 1]

    def head_columns(y, k):
        return pl.ds(pl.multiple_of((y * heads + k) * HEAD_DIM, HEAD_DIM), HEAD_DIM)

    def query_columns(y, k):
        return pl.ds(pl.multiple_of((y * heads + k) * span, span), span)

    def given(kind, part, cols):
        ref = inputs[kind][min(part, 1)]
        return ref.at[:, cols] if part == 0 else ref.at[part - 1, :, cols]

    def valid(where):
        return jnp.logical_and(where >= 0, where < groups)

    units = [(k, b) for k in range(heads) for b in range(2)]
    order = [(k, part) for k in range(heads) for part in parts]

    for c in range(2):
        for where in range(groups):
            @pl.when(where > group)
            def _(c=c, where=where):
                empty = jnp.zeros((2, heads, 2, 2 * rrows, HEAD_DIM), kr.dtype)
                kr[:, :, :, pl.ds((c * groups + where) * 2 * rrows, 2 * rrows), :] = empty
    for ref in (rp, rr, lp, lr):
        ref[...] = jnp.zeros_like(ref)

    barrier = pltpu.get_barrier_semaphore()
    peers = [partner, across] + [
        device((group + i) % groups, y, core) for i in range(1, groups) for y in range(2)
    ]
    for other in peers:
        pl.semaphore_signal(
            barrier, inc=1, device_id={"ctx": other}, device_id_type=pl.DeviceIdType.MESH
        )

    for k, part in order:
        for kind in range(2):
            pltpu.make_async_copy(
                given(kind, part, head_columns(1 - side, k)),
                stack((bp, br), k, part).at[kind], local_sem.at[min(part, 1)],
            ).start()
            pltpu.make_async_copy(
                given(kind, part, head_columns(side, k)),
                pick((kp, kr), k, part).at[kind, side_rows(part, side), :],
                local_sem.at[2 + min(part, 1)],
            ).start()
    wide_own = pl.ds(pl.multiple_of(side * wide, wide), wide)
    wide_far = pl.ds(pl.multiple_of((1 - side) * wide, wide), wide)
    for i, src in enumerate((q, u)):
        pltpu.make_async_copy(src.at[:, :, wide_far], quf.at[i], local_sem.at[4]).start()
        pltpu.make_async_copy(src.at[:, :, wide_own], quh.at[i, side], local_sem.at[5]).start()

    for c in range(2):
        for where in range(groups):
            for y in range(2):
                start = ((c * groups + where) * 2 + y) * rrows
                kpos[pl.ds(start, rrows), :] = device(where, y, c) * rrows + lax.broadcasted_iota(
                    jnp.int32, (rrows, 1), 0
                )

    def landed(ref, i):
        pltpu.make_async_copy(ref, ref, local_sem.at[i]).wait()

    def hello():
        pl.semaphore_wait(barrier, len(peers))

    hello()
    landed(bp, 0)
    landed(br, 1)

    def cross(k, part, kind, y=side):
        src = stack((bp, br), k, part).at[kind]
        dst = pick((kp, kr), k, part).at[kind, side_rows(part, y), :]
        return remote(src, dst, ysend.at[min(part, 1)], yrecv.at[kind, part, k], across)

    def query_cross(i, k, b, y=side):
        cols = pl.ds(k * span, span)
        return remote(
            quf.at[i, b, :, cols], quh.at[i, y, b, :, cols],
            qsend.at[0], qrecv.at[i, k, b], across,
        )

    def shared(k, part, kind):
        ref = pick((kp, kr), k, part).at[kind, core_rows(part, core), :]
        return remote(ref, ref, dsend.at[min(part, 1)], drecv.at[kind, part, k], partner)

    def fanned(part, i):
        return asend_p.at[i] if part == 0 else asend_r.at[i]

    def fan(k, part, kind):
        cross(k, part, kind, 1 - side).wait_recv()
        ref = pick((kp, kr), k, part).at[kind, block_rows(part, core, group), :]
        for i, delta in enumerate(offsets(groups, signs_out(part))):
            if delta == FAR:
                continue
            to = group + delta
            copy = remote(
                ref, ref, fanned(part, i), arecv.at[kind, part, k, group], device(to, side, core)
            )
            pl.when(valid(to))(copy.start)

    def spread(k, part, kind):
        near = pick((kp, kr), k, part).at[kind, side_rows(part, side), :]
        far = stack((bp, br), k, part).at[kind]
        for i, delta in enumerate(offsets(groups, signs_out(part))):
            if delta == FAR:
                continue
            to = group + delta
            sem, got = fanned(part, i), arecv.at[kind, part, k, group]

            @pl.when(valid(to))
            def _(to=to, sem=sem, got=got):
                remote(near, near, sem, got, device(to, side, core)).start()
                remote(far, near, sem, got, device(to, 1 - side, core)).start()

    def came(k, part, kind, origin):
        ref = pick((kp, kr), k, part).at[kind, block_rows(part, core, origin), :]
        return remote(ref, ref, bsend.at[min(part, 1)], arecv.at[kind, part, k, origin], onward)

    def relay(k, part, kind):
        if groups <= FAR:
            return
        origin = group - FAR + 1
        copy = came(k, part, kind, origin)

        @pl.when(jnp.logical_and(origin >= 0, group + 1 < groups))
        def _():
            copy.wait_recv()
            copy.start()

    def arrive(k, part, kind):
        if (k, part) in spread_parts and kind == 0:
            cross(k, part, kind, 1 - side).wait_recv()
        for delta in sorted(offsets(groups, signs_out(part)), key=abs):
            origin = group - delta
            waits = valid(origin)
            if delta == FAR - 1 and groups > FAR:
                waits = jnp.logical_and(waits, group + 1 >= groups)
            pl.when(waits)(came(k, part, kind, origin).wait_recv)
        shared(k, part, kind).start()

    spread_parts = ((0, 0), (0, 1))

    def met(k, part):
        ref = pick((tp, tr), k, part).at[:, core_rows(part, 1 - core), :]
        return remote(
            ref, pick((xp, xr), k, part), csend.at[min(part, 1)], crecv.at[part, k], partner
        )

    def meet(k, part):
        met(k, part).start()

    def total(kind, k, part, where):
        mine = pick((tp, tr), k, part).at[kind, block_rows(part, core, where), :]
        other = pick((xp, xr), k, part).at[kind, half_rows(part, where), :]
        return mine[...] + other[...]

    def returns(part):
        return offsets(groups, signs_back(part)) + [0]

    def returned(part, i):
        return zsend_p.at[i] if part == 0 else zsend_r.at[i]

    def push(k, part, gathers, only=None):
        size = size_of(part)
        passing = stack((lp, lr), k, part)
        more = group + 1 < groups
        for i, delta in enumerate(returns(part)):
            to = group + delta
            cond = valid(to)
            if delta == 1 - FAR and groups > FAR:
                cond = jnp.logical_and(cond, more if gathers else jnp.logical_not(more))
            elif gathers:
                continue
            if only is not None and (delta == -FAR) != only:
                continue
            out = stack((sp, sr), k, part).at[i]
            if delta == -FAR:
                copies = [remote(out, passing, returned(part, i), lrecv.at[part, k], back)]
            else:
                sides = range(2) if delta else (1 - side,)
                copies = [
                    remote(
                        out.at[y], stack((rp, rr), k, part).at[side, group], returned(part, i),
                        zrecv.at[part, k, group], device(to, y, core),
                    )
                    for y in sides
                ]
            wait = remote(out, passing, returned(part, i), lrecv.at[part, k], back)

            @pl.when(cond)
            def _(to=to, out=out, copies=copies, wait=wait):
                if gathers:
                    wait.wait_recv()
                for kind in range(2):
                    value = total(kind, k, part, to)
                    for y in range(2):
                        piece = value[y * size : (y + 1) * size]
                        if gathers:
                            piece = piece + passing[y, kind].astype(jnp.float32)
                        out[y, kind] = piece.astype(jnp.bfloat16)
                for copy in copies:
                    copy.start()

    starts = (0, prows, prows + rrows)

    def finish(k, part):
        got = stack((rp, rr), k, part)
        size = size_of(part)
        for delta in returns(part):
            if delta == -FAR:
                continue
            origin = group - delta
            slot = got.at[:, origin] if delta else got.at[0, origin]
            copy = remote(slot, slot, fanned(part, 0), zrecv.at[part, k, origin], partner)
            pl.when(valid(origin))(copy.wait_recv)
        rows = pl.ds(starts[part], size)
        near = at_row(group * 2 * size + side * size, size)
        for kind in range(2):
            mine = pick((tp, tr), k, part).at[kind, side_rows(part, side), :]
            own = mine[...] + pick((xp, xr), k, part).at[kind, near, :][...]
            out = outputs[kind][min(part, 1)]
            for y in range(2):
                value = jnp.where(side == y, own, jnp.zeros_like(own))
                for origin in range(groups):
                    value = value + got[y, origin, kind].astype(jnp.float32)
                fb[k, kind, y, rows, :] = value
                cols = pl.ds((y * heads + k) * HEAD_DIM, HEAD_DIM)
                dst = out.at[:, cols] if part == 0 else out.at[part - 1, :, cols]
                pltpu.make_async_copy(fb.at[k, kind, y, rows, :], dst, fsem.at[0]).start()

    def drain():
        remote(bp, bp, ysend.at[0], ysend.at[0], across).wait_send()
        remote(br, br, ysend.at[1], ysend.at[1], across).wait_send()
        remote(quf, quf, qsend.at[0], qsend.at[0], across).wait_send()
        ref = kp.at[:, :, core_rows(0, core), :]
        remote(ref, ref, dsend.at[0], dsend.at[0], partner).wait_send()
        ref = kr.at[:, :, :, core_rows(1, core), :]
        remote(ref, ref, dsend.at[1], dsend.at[1], partner).wait_send()
        ref = tp.at[:, :, core_rows(0, 1 - core), :]
        remote(ref, ref, csend.at[0], csend.at[0], partner).wait_send()
        ref = tr.at[:, :, :, core_rows(1, 1 - core), :]
        remote(ref, ref, csend.at[1], csend.at[1], partner).wait_send()
        for part in range(2):
            for i, delta in enumerate(offsets(groups, signs_out(part))):
                if part == 0:
                    ref = kp.at[:, :, block_rows(0, core, group), :]
                else:
                    ref = kr.at[:, :, :, block_rows(1, core, group), :]
                sem = fanned(part, i)
                if delta != FAR:
                    pl.when(valid(group + delta))(remote(ref, ref, sem, sem, across).wait_send)
                    continue
                origin = group - FAR + 1
                if part == 0:
                    ref = kp.at[:, :, block_rows(0, core, origin), :]
                else:
                    ref = kr.at[:, :, :, block_rows(1, core, origin), :]
                sem = bsend.at[part]
                pl.when(jnp.logical_and(origin >= 0, group + 1 < groups))(
                    remote(ref, ref, sem, sem, across).wait_send
                )
            for i, delta in enumerate(returns(part)):
                ref = sp.at[:, i] if part == 0 else sr.at[:, :, i]
                if delta == 0:
                    ref = sp.at[:, i, 0] if part == 0 else sr.at[:, :, i, 0]
                sem = returned(part, i)
                pl.when(valid(group + delta))(remote(ref, ref, sem, sem, across).wait_send)

    def close():
        ref = dq.at[0]
        remote(ref, ref, gsem.at[0], gsem.at[1], across).wait()
        pltpu.make_async_copy(ref, ref, gsem.at[2]).wait()
        pltpu.make_async_copy(fb, fb, fsem.at[0]).wait()

    half = members * rrows
    lanes = 2 * half
    prompt_blocks = kp.shape[2] // block
    resp_blocks = kr.shape[3] // block
    factor = SCALE * LOG2E
    lane = lax.broadcasted_iota(jnp.int32, (1, lanes), 1)
    row_of = lax.rem(lane, rrows)
    first_row = device(group, 0, core) * rrows
    positions = first_row + row_of + jnp.where(lane < half, 0, 2 * rrows)
    row_iota = lax.broadcasted_iota(jnp.int32, (rrows, 1), 0)
    nt = (((1,), (1,)), ((), ()))

    def key_rows(j):
        return pl.ds(pl.multiple_of(j * block, block), block)

    def compute(unit, ticks):
        k, b = units[unit]
        length = lengths[b]
        for source in range(2):
            for g in range(members):
                cols = pl.ds((k * members + g) * HEAD_DIM, HEAD_DIM)
                at = pl.ds(source * half + g * rrows, rrows)
                qs[at, :] = quh[0, source, b, :, cols]
        m_buf[...] = jnp.full_like(m_buf, -jnp.inf)
        l_buf[...] = jnp.zeros_like(l_buf)
        e_buf[...] = jnp.zeros_like(e_buf)
        qt_buf[...] = jnp.zeros_like(qt_buf)
        ticks(0)

        def scores(keys, at, j, causal):
            s = lax.dot_general(keys, qs[...], nt, preferred_element_type=jnp.float32)
            if causal:
                s = jnp.where(kpos[key_rows(j), :] <= positions, s, -jnp.inf)
            s_buf[at, :] = s
            m_buf[...] = jnp.maximum(m_buf[...], jnp.max(s, axis=0, keepdims=True))

        @pl.loop(0, prompt_blocks, unroll=True)
        def _(j):
            scores(kp[0, k, key_rows(j), :], key_rows(j), j, False)

        ticks(1)

        @pl.loop(0, resp_blocks, unroll=True)
        def _(j):
            scores(kr[0, k, b, key_rows(j), :], key_rows(prompt_blocks + j), j, True)

        ticks(2)
        for source in range(2):
            live = first_row + source * 2 * rrows + row_iota < length
            for g in range(members):
                cols = pl.ds((k * members + g) * HEAD_DIM, HEAD_DIM)
                at = pl.ds(source * half + g * rrows, rrows)
                rows = quh[1, source, b, :, cols]
                us[at, :] = jnp.where(live, rows, jnp.zeros_like(rows))
        shift = m_buf[...] * factor

        def weights(vals, at):
            p = jnp.exp2(s_buf[at, :] * factor - shift)
            d = lax.dot_general(vals, us[...], nt, preferred_element_type=jnp.float32)
            l_buf[...] += jnp.sum(p, axis=0, keepdims=True)
            e_buf[...] += jnp.sum(p * d, axis=0, keepdims=True)
            s_buf[at, :] = p
            d_buf[at, :] = d

        @pl.loop(0, prompt_blocks, unroll=True)
        def _(j):
            weights(kp[1, k, key_rows(j), :], key_rows(j))

        ticks(3)

        @pl.loop(0, resp_blocks, unroll=True)
        def _(j):
            weights(kr[1, k, b, key_rows(j), :], key_rows(prompt_blocks + j))

        ticks(4)
        inverse = 1.0 / l_buf[...]
        delta = e_buf[...] * inverse

        def grads(keys, at):
            p = s_buf[at, :] * inverse
            ds = (p * (d_buf[at, :] - delta)).astype(jnp.bfloat16)
            dv = jnp.dot(p.astype(jnp.bfloat16), us[...], preferred_element_type=jnp.float32)
            dk = jnp.dot(ds, qs[...], preferred_element_type=jnp.float32) * SCALE
            qt_buf[...] += jnp.dot(keys.T, ds, preferred_element_type=jnp.float32)
            return dk, dv

        @pl.loop(0, prompt_blocks, unroll=True)
        def _(j):
            at = key_rows(j)
            pair = grads(kp[0, k, at, :], at)
            for kind in range(2):
                if b == 0:
                    tp[kind, k, at, :] = pair[kind]
                else:
                    tp[kind, k, at, :] += pair[kind]

        ticks(5)

        @pl.loop(0, resp_blocks, unroll=True)
        def _(j):
            at = key_rows(j)
            pair = grads(kr[0, k, b, at, :], key_rows(prompt_blocks + j))
            for kind in range(2):
                tr[kind, k, b, at, :] = pair[kind]

        ticks(6)
        result = (qt_buf[...].T * SCALE).astype(jnp.bfloat16)
        for source in range(2):
            for g in range(members):
                start = source * half + g * rrows
                dq[source, b, :, pl.ds((k * members + g) * HEAD_DIM, HEAD_DIM)] = result[
                    start : start + rrows
                ]
        cols = pl.ds(k * span, span)
        to = query_columns(side, k)
        remote(
            dq.at[1 - side, b, :, cols], gq.at[b, :, to], gsem.at[0], gsem.at[1], across
        ).start()
        pltpu.make_async_copy(dq.at[side, b, :, cols], gq.at[b, :, to], gsem.at[2]).start()

    def needs(unit):
        k, b = units[unit]
        return [(k, 0), (k, 1)] if b == 0 else [(k, 2)]

    def yields(unit):
        k, b = units[unit]
        return [(k, 1)] if b == 0 else [(k, 0), (k, 2)]

    def ready(unit):
        k, b = units[unit]
        for pair in needs(unit):
            shared(*pair, 0).wait_recv()
        query_cross(0, k, b, 1 - side).wait_recv()

    last = len(units) - 1
    landed(kp.at[:, :, side_rows(0, side), :], 2)
    landed(kr.at[:, :, :, side_rows(1, side), :], 3)
    for pair in spread_parts:
        spread(*pair, 0)
        cross(*pair, 0).start()
    for pair in spread_parts:
        cross(*pair, 1).start()
    for kind in range(2):
        cross(0, 2, kind).start()
    landed(quf, 4)
    query_cross(0, *units[0]).start()
    for kind in range(2):
        for pair in needs(2):
            cross(*pair, kind).start()
    query_cross(1, *units[0]).start()
    for unit in range(3, last + 1):
        for kind in range(2):
            for pair in needs(unit):
                cross(*pair, kind).start()
    for i in range(2):
        query_cross(i, *units[1]).start()
    for unit in range(2, last + 1):
        for i in range(2):
            query_cross(i, *units[unit]).start()
    for pair in spread_parts:
        fan(*pair, 1)
    for pair in spread_parts:
        relay(*pair, 0)
    for kind in range(2):
        fan(0, 2, kind)
    for pair in spread_parts:
        arrive(*pair, 0)
    for pair in spread_parts:
        relay(*pair, 1)
    landed(quh.at[:, side], 5)
    ready(0)
    for unit in range(last + 1):
        k, b = units[unit]

        def ticks(at, unit=unit, k=k, b=b):
            if at == 0 and unit == 0:
                for kind in range(2):
                    relay(0, 2, kind)
            if unit == 0 and at == 1:
                for kind in range(2):
                    for pair in needs(2):
                        fan(*pair, kind)
                arrive(0, 0, 1)
            if at == 2:
                if unit == 0:
                    arrive(0, 1, 1)
                for pair in needs(unit):
                    shared(*pair, 1).wait_recv()
                query_cross(1, k, b, 1 - side).wait_recv()
            if at == 3 and unit + 3 <= last:
                for pair in needs(unit + 3):
                    for kind in range(2):
                        fan(*pair, kind)
            if at in (4, 5) and unit < last:
                for pair in needs(unit + 1):
                    arrive(*pair, at - 4)
            if at == 2 and unit > 0:
                for pair in yields(unit - 1):
                    met(*pair).wait_recv()
                    push(*pair, False)
            if at == 4 and unit > 1:
                for pair in yields(unit - 2):
                    push(*pair, True)
            if at == 5 and b == 1:
                meet(k, 0)
            if at == 6:
                meet(k, b + 1)
                if unit + 2 <= last:
                    for kind in range(2):
                        for pair in needs(unit + 2):
                            relay(*pair, kind)
                if unit == last:
                    for pair in yields(unit - 1):
                        push(*pair, True)
                    met(k, 0).wait_recv()
                    push(k, 0, False, True)

        compute(unit, ticks)
        if unit < last:
            ready(unit + 1)
    for pair in yields(last):
        if pair[1] > 0:
            met(*pair).wait_recv()
            push(*pair, False, True)
    for pair in yields(last):
        push(*pair, False, False)
    for pair in yields(last):
        push(*pair, True)
    for unit in range(last + 1):
        for pair in yields(unit):
            finish(*pair)
    drain()
    close()


def key_block(prompt, resp):
    size = 256
    while prompt % size or resp % size:
        size //= 2
    return size


def chunks_of(array):
    return 4 if array.size > 1 << 18 else 1


def settle_kernel(*refs):
    count = (len(refs) - 2) // 4
    sources, targets = refs[:count], refs[count : 2 * count]
    holds, wides = refs[2 * count : 3 * count], refs[3 * count : 4 * count]
    taken, given = refs[4 * count :]
    pieces = []
    for source, target, hold, wide in zip(sources, targets, holds, wides):
        chunks = chunks_of(source)
        step = source.shape[-1] // chunks
        for c in range(chunks):
            cut = (slice(None),) * (len(source.shape) - 1) + (pl.ds(c * step, step),)
            i = len(pieces)
            taking = pltpu.make_async_copy(source.at[cut], hold.at[cut], taken.at[i])
            taking.start()
            giving = pltpu.make_async_copy(wide.at[cut], target.at[cut], given.at[i])
            pieces.append((taking, giving, hold, wide, cut))
    for taking, giving, hold, wide, cut in pieces:
        taking.wait()
        wide[cut] = hold[cut].astype(wide.dtype)
        giving.start()
    for piece in pieces:
        piece[1].wait()


def settle(*arrays):
    hbm = pl.BlockSpec(memory_space=pl.ANY)
    dma = pltpu.SemaphoreType.DMA
    pieces = sum(chunks_of(x) for x in arrays)
    return pl.pallas_call(
        settle_kernel,
        out_shape=tuple(jax.ShapeDtypeStruct(x.shape, jnp.float32) for x in arrays),
        in_specs=[hbm] * len(arrays),
        out_specs=(hbm,) * len(arrays),
        scratch_shapes=[pltpu.VMEM(x.shape, x.dtype) for x in arrays]
        + [pltpu.VMEM(x.shape, jnp.float32) for x in arrays]
        + [dma((pieces,)), dma((pieces,))],
        compiler_params=pltpu.CompilerParams(vmem_limit_bytes=60 * MIB),
        name="settle",
    )(*arrays)


def local(prompt_keys, prompt_values, queries, resp_keys, resp_values, cotangent, lengths):
    devices = lax.axis_size("ctx")
    groups = devices // 4
    prows, columns = prompt_keys.shape
    rows, wide = queries.shape[1], queries.shape[2] // 2
    heads = columns // 2 // HEAD_DIM
    prompt, resp = prows * devices, rows * devices
    smem = pl.BlockSpec(memory_space=pltpu.SMEM)
    hbm = pl.BlockSpec(memory_space=pl.ANY)
    shape = jax.ShapeDtypeStruct
    bf16, f32 = jnp.bfloat16, jnp.float32
    vmem, dma = pltpu.VMEM, pltpu.SemaphoreType.DMA
    block = key_block(prompt, resp)
    lanes = 2 * rows * (wide // HEAD_DIM) // heads
    total = prompt + resp
    both, one = len(offsets(groups, (1, -1))), len(offsets(groups, (1,)))
    outs = pl.pallas_call(
        functools.partial(fused_kernel, groups, block),
        out_shape=(
            shape((2, rows, 2 * wide), bf16),
            shape((2, rows, columns), f32), shape((2, rows, columns), f32),
            shape((prows, columns), f32), shape((prows, columns), f32),
        ),
        in_specs=[smem] + [hbm] * 6,
        out_specs=(hbm,) * 5,
        scratch_shapes=[
            vmem((2, heads, prompt, HEAD_DIM), bf16),
            vmem((2, heads, 2, resp, HEAD_DIM), bf16),
            vmem((heads, 2, prows, HEAD_DIM), bf16),
            vmem((heads, 2, 2, rows, HEAD_DIM), bf16),
            vmem((resp, 1), jnp.int32),
            vmem((2, 2, 2, rows, wide), bf16), vmem((2, 2, rows, wide), bf16),
            vmem((lanes, HEAD_DIM), bf16), vmem((lanes, HEAD_DIM), bf16),
            vmem((total, lanes), f32), vmem((total, lanes), f32),
            vmem((HEAD_DIM, lanes), f32),
            vmem((1, lanes), f32), vmem((1, lanes), f32), vmem((1, lanes), f32),
            vmem((2, heads, prompt, HEAD_DIM), f32),
            vmem((2, heads, 2, resp, HEAD_DIM), f32),
            vmem((2, heads, prompt // 2, HEAD_DIM), f32),
            vmem((2, heads, 2, resp // 2, HEAD_DIM), f32),
            vmem((heads, both + 1, 2, 2, prows, HEAD_DIM), bf16),
            vmem((heads, 2, one + 1, 2, 2, rows, HEAD_DIM), bf16),
            vmem((heads, 2, groups, 2, prows, HEAD_DIM), bf16),
            vmem((heads, 2, 2, groups, 2, rows, HEAD_DIM), bf16),
            vmem((heads, 2, 2, prows, HEAD_DIM), bf16),
            vmem((heads, 2, 2, 2, rows, HEAD_DIM), bf16),
            vmem((heads, 2, 2, prows + 2 * rows, HEAD_DIM), f32),
            vmem((2, 2, rows, wide), bf16),
            dma((6,)), dma((2,)), dma((2, 3, heads)), dma((1,)), dma((2, heads, 2)),
            dma((both,)), dma((one,)), dma((2, 3, heads, groups)), dma((2,)), dma((3, heads)),
            dma((2,)), dma((2, 3, heads)), dma((2,)), dma((3, heads)),
            dma((both + 1,)), dma((one + 1,)), dma((3, heads, groups)), dma((1,)), dma((3,)),
        ],
        compiler_params=pltpu.CompilerParams(
            collective_id=0, has_side_effects=True, vmem_limit_bytes=60 * MIB
        ),
        name="fused",
    )(lengths, prompt_keys, prompt_values, resp_keys, resp_values, queries, cotangent)
    return settle(*outs)


def solution(mesh):
    placed = (
        P(("pairs", "ctx"), None),
        P(("pairs", "ctx"), None),
        P("pairs", "ctx", None),
        P("pairs", "ctx", None),
        P("pairs", "ctx", None),
        P("pairs", "ctx", None),
        P("pairs"),
    )
    return jax.shard_map(
        local,
        mesh=mesh,
        in_specs=placed,
        out_specs=(
            P("pairs", "ctx", None),
            P("pairs", "ctx", None),
            P("pairs", "ctx", None),
            P(("pairs", "ctx"), None),
            P(("pairs", "ctx"), None),
        ),
        check_vma=False,
    )
```
